64 devices in a mesh: rep: 4 (over x, y), dp: 16 (over z, core).
Axes of the slice: x: 2, y: 2, z: 8, core: 2. Of those that a mesh axis runs over, the one named last changes fastest.
The devices are a block of a 4x4x8 slice.
Arguments:
- g_w_gate: bfloat16 [64, 2, 512, 8192], P(('rep', 'dp')), parts along dimension 0
- g_w_up: bfloat16 [64, 2, 512, 8192], P(('rep', 'dp')), parts along dimension 0
- g_w_down: bfloat16 [64, 2, 8192, 512], P(('rep', 'dp')), parts along dimension 0
- w_gate: bfloat16 [2, 512, 8192], replicated
- w_up: bfloat16 [2, 512, 8192], replicated
- w_down: bfloat16 [2, 8192, 512], replicated
- m_w_gate: float32 [2, 512, 8192], P(None, 'dp')
- m_w_up: float32 [2, 512, 8192], P(None, 'dp')
- m_w_down: float32 [2, 8192, 512], P(None, 'dp')
- v_w_gate: float32 [2, 512, 8192], P(None, 'dp')
- v_w_up: float32 [2, 512, 8192], P(None, 'dp')
- v_w_down: float32 [2, 8192, 512], P(None, 'dp')
Outputs:
- output 1: bfloat16 [8, 512, 8192], P('rep'), parts along dimension 0
- output 2: bfloat16 [8, 512, 8192], P('rep'), parts along dimension 0
- output 3: bfloat16 [8, 8192, 512], P('rep'), parts along dimension 0
- output 4: float32 [8, 512, 8192], P('rep', 'dp'), parts along dimension 0
- output 5: float32 [8, 512, 8192], P('rep', 'dp'), parts along dimension 0
- output 6: float32 [8, 8192, 512], P('rep', 'dp'), parts along dimension 0
- output 7: float32 [8, 512, 8192], P('rep', 'dp'), parts along dimension 0
- output 8: float32 [8, 512, 8192], P('rep', 'dp'), parts along dimension 0
- output 9: float32 [8, 8192, 512], P('rep', 'dp'), parts along dimension 0
There are 4 independent parts. The reference program is written for one: setup_inputs(seed, part) draws one part's arguments, and reference() takes and returns one part's arrays. A program takes and returns all parts, laid end to end along the dimension named above; an argument that names none is the same for every part.
All inputs are finite; a program needn't handle non-finite values.
Results may differ from the reference program's by a relative error of at most 0.022.
Values are sent between devices in bfloat16 or wider.
A program may use at most 768 MiB of HBM per device.

```python
import jax
import jax.numpy as jnp
from jax import lax

DEVICES = 16
D = 512
FF = 8192
LAYERS = 2
NAMES = ("w_gate", "w_up", "w_down")
SHAPES = {"w_gate": (LAYERS, D, FF), "w_up": (LAYERS, D, FF), "w_down": (LAYERS, FF, D)}


def setup_inputs(seed: int = 0, part: int = 0) -> dict:
    kz, *keys = jax.random.split(jax.random.key(seed), 1 + 5 * len(NAMES))
    loud = 2.0 ** jax.random.uniform(kz, (), jnp.float32, -1.0, 1.0)
    drawn = {}
    for name, key, both in zip(NAMES, keys[:3], keys[3:6], strict=True):
        own = jax.random.normal(jax.random.fold_in(key, part), (DEVICES, *SHAPES[name]), jnp.float32)
        shared = jax.random.normal(jax.random.fold_in(both, part), SHAPES[name], jnp.float32)
        drawn["g_" + name] = (loud * (0.7 * shared / DEVICES + 0.7 * own * DEVICES**-0.5)).astype(jnp.bfloat16)
    for name, key in zip(NAMES, keys[6:9], strict=True):
        drawn[name] = (jax.random.normal(key, SHAPES[name], jnp.float32) * SHAPES[name][1] ** -0.5).astype(jnp.bfloat16)
    for name, key in zip(NAMES, keys[9:12], strict=True):
        drawn["m_" + name] = loud * 0.5 * jax.random.normal(key, SHAPES[name], jnp.float32)
    for name, key in zip(NAMES, keys[12:15], strict=True):
        drawn["v_" + name] = loud * loud * jax.random.uniform(key, SHAPES[name], jnp.float32, 0.5, 1.5)
    return drawn


def adamw(w, m, v, g):
    m = 0.9 * m + 0.1 * g
    v = 0.95 * v + 0.05 * g * g
    step = m * lax.rsqrt(v + 1e-8) + 0.1 * w
    return (w - 0.02 * step).astype(jnp.bfloat16), m, v


def clipped(gradients, sum_of_squares, count):
    factor = jnp.minimum(1.0, 0.5 * lax.rsqrt(sum_of_squares / count + 1e-30))
    return [g * factor for g in gradients]


def reference(g_w_gate, g_w_up, g_w_down, w_gate, w_up, w_down, m_w_gate, m_w_up, m_w_down, v_w_gate, v_w_up, v_w_down):
    def total(terms):
        return lax.scan(lambda so_far, term: (so_far + term.astype(jnp.float32), None), jnp.zeros(terms.shape[1:], jnp.float32), terms)[0]

    gradients = [total(terms).astype(jnp.bfloat16).astype(jnp.float32) for terms in (g_w_gate, g_w_up, g_w_down)]
    gradients = clipped(gradients, sum(jnp.sum(g * g) for g in gradients), sum(g.size for g in gradients))
    new = [
        adamw(w.astype(jnp.float32), m, v, g)
        for w, m, v, g in zip((w_gate, w_up, w_down), (m_w_gate, m_w_up, m_w_down), (v_w_gate, v_w_up, v_w_down), gradients, strict=True)
    ]
    return tuple(one[which] for which in range(3) for one in new)
```

```python
import functools

import jax
import jax.numpy as jnp
from jax import lax
from jax.experimental import pallas as pl
from jax.experimental.pallas import tpu as pltpu
from jax.sharding import PartitionSpec as P

MESH = pl.DeviceIdType.MESH
CORES = 2
PLUS, MINUS = 0, 1


def pieces_of(layers):
    return [(a, layer) for layer in range(layers) for a in range(3)]


def plan(n, layers):
    half = n // 2
    mine = lambda way: [q for q in pieces_of(layers) if (q[1] % 2 == 0) == (way == PLUS)]
    other = lambda way: [q for q in pieces_of(layers) if (q[1] % 2 == 0) != (way == PLUS)]
    queue = {}
    for way in (PLUS, MINUS):
        sends = [(way, half, q) for q in mine(way)]
        for d in range(half - 1, 0, -1):
            order = (other(way) + mine(way)) if d > 1 else (other(PLUS) + mine(PLUS))
            sends += [(way, d, q) for q in order]
        queue[way] = sends
    items = [s for pair in zip(queue[PLUS], queue[MINUS], strict=True) for s in pair]
    finals = [(None, 0, q) for q in other(PLUS) + mine(PLUS)]
    arrives = {}
    fresh = {}
    count = [0, 0]

    def slot(q):
        kind = int(q[0] == 2)
        count[kind] += 1
        return kind, count[kind] - 1

    for s in items:
        arrives[s] = slot(s[2])
    for s in items:
        way, d, q = s
        if (way, d + 1, q) not in arrives:
            fresh[s] = slot(q)
    return items, finals, arrives, fresh, count


def kernel(n, count_all, *refs):
    (gg, gu, gd, wg, wu, wd, mg, mu, md, vg, vu, vd) = refs[:12]
    (tg, tu, td, omg, omu, omd, ovg, ovu, ovd, xw, xd) = refs[12:23]
    (rw, rd, ow, od, pw, pd, mvw, mvd, bw, bd, ww, wwd, squares) = refs[23:36]
    (rs_send, rs_recv, x_send, x_recv, st_sem, ag_send, ag_recv, y_send, y_recv, sq_send, sq_recv, in_sem, out_sem) = refs[36:]

    g, w, m, v = (gg, gu, gd), (wg, wu, wd), (mg, mu, md), (vg, vu, vd)
    t, om, ov = (tg, tu, td), (omg, omu, omd), (ovg, ovu, ovd)
    layers = m[0].shape[0]
    rows = [a.shape[1] for a in m]
    items, finals, arrives, fresh, _ = plan(n, layers)
    pieces = pieces_of(layers)
    todo = items + finals
    half = n // 2
    devices = n * CORES

    me = lax.axis_index("dp")
    z, c = me // CORES, me % CORES
    at = lambda chip, core: lax.rem(chip + n, n) * CORES + core
    partner = at(z, 1 - c)
    ahead = {PLUS: at(z + 1, c), MINUS: at(z - 1, c)}
    step = {PLUS: 1, MINUS: -1}

    def block(ref, q, owner):
        a, layer = q
        r = pl.ds(pl.multiple_of(owner * rows[a], rows[a]), rows[a])
        return ref[a].at[layer, r]

    def term(q, owner):
        a, layer = q
        r = pl.ds(pl.multiple_of(owner * rows[a], rows[a]), rows[a])
        return g[a].at[0, layer, r]

    def remote(src, dst, send, recv, to):
        return pltpu.make_async_remote_copy(src_ref=src, dst_ref=dst, send_sem=send, recv_sem=recv, device_id={"dp": to}, device_id_type=MESH)

    barrier = pltpu.get_barrier_semaphore()
    for j in range(1, devices):
        pl.semaphore_signal(barrier, inc=1, device_id={"dp": lax.rem(me + j, devices)}, device_id_type=MESH)
    pl.semaphore_wait(barrier, devices - 1)

    x_at = []
    seen = [0, 0]
    for _, _, q in todo:
        kind = int(q[0] == 2)
        x_at.append((kind, seen[kind]))
        seen[kind] += 1
    xs, st_own, st_other, landed = (xw, xd), (ow, od), (pw, pd), (rw, rd)
    depth = [ow.shape[0], od.shape[0]]

    def target(way, d):
        return z if way is None else z + step[way] * d

    def exchange(i):
        way, d, q = todo[i]
        kind, k = x_at[i]
        return remote(term(q, at(target(way, d), 1 - c)), xs[kind].at[k], x_send.at[i], x_recv.at[i], partner)

    def stage(i):
        way, d, q = todo[i]
        kind, k = x_at[i]
        s = k % depth[kind]
        sem = kind * depth[0] + s
        return (
            pltpu.make_async_copy(term(q, at(target(way, d), c)), st_own[kind].at[s], st_sem.at[0, sem]),
            pltpu.make_async_copy(xs[kind].at[k], st_other[kind].at[s], st_sem.at[1, sem]),
        )

    def stage_start(i):
        exchange(i).wait_recv()
        for copy in stage(i):
            copy.start()

    def slices(kind, shape, size):
        if kind:
            r = max(16, size // shape[1])
            return shape[0] // r, lambda j: (pl.ds(pl.multiple_of(j * r, r), r), slice(None))
        cols = max(128, size // shape[0])
        return shape[1] // cols, lambda j: (slice(None), pl.ds(pl.multiple_of(j * cols, cols), cols))

    def added(dst, terms, kind, total=None):
        cuts, cut = slices(kind, dst.shape, 16384)

        def one(j, acc):
            part = cut(j)
            s = terms[0][part].astype(jnp.float32)
            for r in terms[1:]:
                s = s + r[part].astype(jnp.float32)
            s = s.astype(dst.dtype)
            dst[part] = s
            if acc is None:
                return None
            s = s.astype(jnp.float32)
            s = s * s
            s = jnp.sum(s.reshape(s.shape[0] // 8, 8, s.shape[1]), axis=0)
            for k in range(s.shape[1] // 128):
                acc = acc + s[:, k * 128 : (k + 1) * 128]
            return acc

        return lax.fori_loop(0, cuts, one, total)

    def ring(s):
        way, d, q = s
        kind, k = fresh[s] if s in fresh else arrives[(way, d + 1, q)]
        to_kind, to = arrives[s]
        i = items.index(s)
        return remote(landed[kind].at[k], landed[to_kind].at[to], rs_send.at[i], rs_recv.at[i], ahead[way])

    window = 12
    for i in range(window):
        exchange(i).start()
    reach = 2
    for i in range(reach):
        stage_start(i)
    moments = [(m, mvw, mvd, 0), (v, mvw, mvd, 1)]

    def held(which, q):
        a, layer = q
        if a == 2:
            return mvd.at[which, layer]
        return mvw.at[which, a * layers + layer]

    def weight(q):
        a, layer = q
        return bd.at[layer] if a == 2 else bw.at[a * layers + layer]

    def fresh_weight(q):
        a, layer = q
        return wwd.at[layer] if a == 2 else ww.at[a * layers + layer]

    def load_state(e):
        q = pieces[e]
        a, layer = q
        return (
            pltpu.make_async_copy(m[a].at[layer], held(0, q), in_sem.at[0, e]),
            pltpu.make_async_copy(v[a].at[layer], held(1, q), in_sem.at[1, e]),
            pltpu.make_async_copy(block(w, q, me), weight(q), in_sem.at[2, e]),
        )

    total = jnp.zeros((8, 128), jnp.float32)
    for i, s in enumerate(todo):
        way, d, q = s
        kind, k = x_at[i]
        for copy in stage(i):
            copy.wait()
        terms = [st_own[kind].at[k % depth[kind]], st_other[kind].at[k % depth[kind]]]
        if way is not None:
            if s not in fresh:
                before = (way, d + 1, q)
                ring(before).wait_recv()
                ak, ai = arrives[before]
                terms.append(landed[ak].at[ai])
                dst = landed[ak].at[ai]
            else:
                fk, fi = fresh[s]
                dst = landed[fk].at[fi]
            added(dst, terms, kind)
            ring(s).start()
        else:
            for w_ in (PLUS, MINUS):
                ring((w_, 1, q)).wait_recv()
                ak, ai = arrives[(w_, 1, q)]
                terms.append(landed[ak].at[ai])
            total = added(fresh_weight(q), terms, kind, total)
        if i + window < len(todo):
            exchange(i + window).start()
        if i + reach < len(todo):
            stage_start(i + reach)
        if 8 <= i < 8 + len(pieces):
            for copy in load_state(i - 8):
                copy.start()

    squares[me] = total

    def share(j, sender):
        to = lax.rem(me + j, devices)
        return remote(squares.at[sender], squares.at[sender], sq_send.at[j - 1], sq_recv.at[j - 1], to)

    for j in range(1, devices):
        share(j, me).start()
    for i in range(len(todo)):
        exchange(i).wait_send()
    for s in items:
        ring(s).wait_send()
    for e in range(len(pieces)):
        for copy in load_state(e):
            copy.wait()
    for j in range(1, devices):
        share(j, lax.rem(me - j + devices, devices)).wait_recv()
    everyone = jnp.sum(jnp.sum(squares[...], axis=0), axis=(0, 1), keepdims=True)
    factor = jnp.minimum(1.0, 0.5 * lax.rsqrt(jnp.broadcast_to(everyone, (8, 128)) / count_all + 1e-30))[0:1, 0:1]

    def stepped(q):
        kind = int(q[0] == 2)
        wn, mr, vr, wr = fresh_weight(q), held(0, q), held(1, q), weight(q)
        cuts, cut = slices(kind, wn.shape, 8192)

        def one(j, _):
            part = cut(j)
            grad = wn[part].astype(jnp.float32) * factor
            mm = 0.9 * mr[part] + 0.1 * grad
            vv = 0.95 * vr[part] + 0.05 * grad * grad
            mr[part] = mm
            vr[part] = vv
            old = wr[part].astype(jnp.float32)
            wn[part] = (old - 0.02 * (mm * lax.rsqrt(vv + 1e-8) + 0.1 * old)).astype(wn.dtype)
            return None

        lax.fori_loop(0, cuts, one, None)

    order = other_first = [q for q in pieces if q[1] % 2] + [q for q in pieces if not q[1] % 2]
    hops = {way: [(way, h, q) for h in range(1, half) for q in order] for way in (PLUS, MINUS)}
    for way in (PLUS, MINUS):
        hops[way] += [(way, half, q) for q in order if (q[1] % 2 == 1) == (way == PLUS)]
    gathers = [s for pair in zip(hops[PLUS], hops[MINUS], strict=True) for s in pair]

    def pass_on(s, arriving):
        way, h, q = s
        owner = at(z - step[way] * (h if arriving else h - 1), c)
        i = gathers.index(s)
        src = fresh_weight(q) if h == 1 and not arriving else block(t, q, owner)
        return remote(src, block(t, q, owner), ag_send.at[i], ag_recv.at[i], ahead[way])

    def across(i, arriving):
        core = 1 - c if arriving else c
        if i < len(gathers):
            way, h, q = gathers[i]
            owner = at(z - step[way] * h, core)
            src = block(t, q, owner)
        else:
            q = order[i - len(gathers)]
            owner = at(z, core)
            src = block(t, q, owner) if arriving else fresh_weight(q)
        return remote(src, block(t, q, owner), y_send.at[i], y_recv.at[i], partner)

    def results(e):
        q = pieces[e]
        a, layer = q
        return (
            pltpu.make_async_copy(held(0, q), om[a].at[layer], out_sem.at[0, e]),
            pltpu.make_async_copy(held(1, q), ov[a].at[layer], out_sem.at[1, e]),
            pltpu.make_async_copy(fresh_weight(q), block(t, q, me), out_sem.at[2, e]),
        )

    for q in order:
        stepped(q)
        for way in (PLUS, MINUS):
            pass_on((way, 1, q), False).start()
        across(len(gathers) + order.index(q), False).start()
        for copy in results(pieces.index(q)):
            copy.start()
    for i, s in enumerate(gathers):
        way, h, q = s
        pass_on(s, True).wait_recv()
        if (way, h + 1, q) in gathers:
            pass_on((way, h + 1, q), False).start()
        across(i, False).start()
    for j in range(1, devices):
        share(j, me).wait_send()
    for e in range(len(pieces)):
        for copy in results(e):
            copy.wait()
    for s in gathers:
        pass_on(s, False).wait_send()
    for i in range(len(gathers) + len(order)):
        across(i, False).wait_send()
    for i in range(len(gathers) + len(order)):
        across(i, True).wait_recv()


def solution(mesh):
    devices = mesh.shape["dp"]
    n = devices // CORES

    def step(*arrays):
        terms, weights, m, v = (arrays[i : i + 3] for i in (0, 3, 6, 9))
        layers = m[0].shape[0]
        items, finals, _, _, count = plan(n, layers)
        todo = items + finals
        wide, down = m[0].shape[1:], m[2].shape[1:]
        n_down = sum(q[0] == 2 for _, _, q in todo)
        hbm = pl.BlockSpec(memory_space=pl.ANY)
        bf, f32 = jnp.bfloat16, jnp.float32
        dma = pltpu.SemaphoreType.DMA
        sizes = devices * sum(one.size for one in m)
        pieces = len(pieces_of(layers))
        out = pl.pallas_call(
            functools.partial(kernel, n, sizes),
            out_shape=[jax.ShapeDtypeStruct(w.shape, bf) for w in weights]
            + [jax.ShapeDtypeStruct(one.shape, f32) for one in (*m, *v)]
            + [jax.ShapeDtypeStruct((len(todo) - n_down, *wide), bf), jax.ShapeDtypeStruct((n_down, *down), bf)],
            in_specs=[hbm] * 12,
            out_specs=[hbm] * 11,
            scratch_shapes=[
                pltpu.VMEM((count[0], *wide), bf),
                pltpu.VMEM((count[1], *down), bf),
                pltpu.VMEM((4, *wide), bf),
                pltpu.VMEM((2, *down), bf),
                pltpu.VMEM((4, *wide), bf),
                pltpu.VMEM((2, *down), bf),
                pltpu.VMEM((2, 2 * layers, *wide), f32),
                pltpu.VMEM((2, layers, *down), f32),
                pltpu.VMEM((2 * layers, *wide), bf),
                pltpu.VMEM((layers, *down), bf),
                pltpu.VMEM((2 * layers, *wide), bf),
                pltpu.VMEM((layers, *down), bf),
                pltpu.VMEM((devices, 8, 128), f32),
                dma((len(items),)),
                dma((len(items),)),
                dma((len(todo),)),
                dma((len(todo),)),
                dma((2, 6)),
                dma((len(items),)),
                dma((len(items),)),
                dma((len(todo),)),
                dma((len(todo),)),
                dma((devices - 1,)),
                dma((devices - 1,)),
                dma((3, pieces)),
                dma((3, pieces)),
            ],
            compiler_params=pltpu.CompilerParams(collective_id=0, has_side_effects=True, vmem_limit_bytes=60 * 2**20),
        )(*(t for t in terms), *weights, *m, *v)
        return tuple(out[:9])

    all_of, cut = P(None, None, None), P(None, "dp", None)
    return jax.shard_map(
        step,
        mesh=mesh,
        in_specs=(P(("rep", "dp"), None, None, None),) * 3 + (all_of,) * 3 + (cut,) * 6,
        out_specs=(P("rep", None, None),) * 3 + (P("rep", "dp", None),) * 6,
        check_vma=False,
    )
```

```python
import functools

import jax
import jax.numpy as jnp
from jax import lax
from jax.experimental import pallas as pl
from jax.experimental.pallas import tpu as pltpu
from jax.sharding import PartitionSpec as P


MESH = pl.DeviceIdType.MESH
CORES = 2
PLUS, MINUS = 0, 1


def pieces_of(layers):
    return [(a, layer) for layer in range(layers) for a in range(3)]


def plan(n, layers):
    half = n // 2
    mine = lambda way: [q for q in pieces_of(layers) if (q[1] % 2 == 0) == (way == PLUS)]
    other = lambda way: [q for q in pieces_of(layers) if (q[1] % 2 == 0) != (way == PLUS)]
    queue = {}
    for way in (PLUS, MINUS):
        sends = [(way, half, q) for q in mine(way)]
        for d in range(half - 1, 0, -1):
            order = (other(way) + mine(way)) if d > 1 else (other(PLUS) + mine(PLUS))
            sends += [(way, d, q) for q in order]
        queue[way] = sends
    items = [s for pair in zip(queue[PLUS], queue[MINUS], strict=True) for s in pair]
    finals = [(None, 0, q) for q in other(PLUS) + mine(PLUS)]
    arrives = {}
    fresh = {}
    count = [0, 0]

    def slot(q):
        kind = int(q[0] == 2)
        count[kind] += 1
        return kind, count[kind] - 1

    for s in items:
        arrives[s] = slot(s[2])
    for s in items:
        way, d, q = s
        if (way, d + 1, q) not in arrives:
            fresh[s] = slot(q)
    return items, finals, arrives, fresh, count


def last_hop(way, layers):
    return [q for q in pieces_of(layers) if (q[1] % 2 == 1) == (way == PLUS)]


def last_slot(way, layers, q):
    kind = int(q[0] == 2)
    return kind, [p for p in last_hop(way, layers) if int(p[0] == 2) == kind].index(q)


def kernel(n, count_all, *refs):
    (gg, gu, gd, wg, wu, wd, mg, mu, md, vg, vu, vd) = refs[:12]
    (tg, tu, td, omg, omu, omd, ovg, ovu, ovd, xw, xd) = refs[12:23]
    last = {PLUS: refs[23:25], MINUS: refs[25:27]}
    refs = refs[27:]
    (rw, rd, ow, od, pw, pd, mvw, mvd, bw, bd, ww, wwd, squares) = refs[:13]
    (rs_send, rs_recv, x_send, x_recv, st_sem, ag_send, ag_recv, y_send, y_recv, sq_send, sq_recv, in_sem, out_sem) = refs[13:]

    g, w, m, v = (gg, gu, gd), (wg, wu, wd), (mg, mu, md), (vg, vu, vd)
    t, om, ov = (tg, tu, td), (omg, omu, omd), (ovg, ovu, ovd)
    layers = m[0].shape[0]
    rows = [a.shape[1] for a in m]
    items, finals, arrives, fresh, _ = plan(n, layers)
    pieces = pieces_of(layers)
    todo = items + finals
    half = n // 2
    devices = n * CORES

    me = lax.axis_index("dp")
    z, c = me // CORES, me % CORES
    at = lambda chip, core: lax.rem(chip + n, n) * CORES + core
    partner = at(z, 1 - c)
    ahead = {PLUS: at(z + 1, c), MINUS: at(z - 1, c)}
    step = {PLUS: 1, MINUS: -1}

    def block(ref, q, owner):
        a, layer = q
        r = pl.ds(pl.multiple_of(owner * rows[a], rows[a]), rows[a])
        return ref[a].at[layer, r]

    def term(q, owner):
        a, layer = q
        r = pl.ds(pl.multiple_of(owner * rows[a], rows[a]), rows[a])
        return g[a].at[0, layer, r]

    def remote(src, dst, send, recv, to):
        return pltpu.make_async_remote_copy(src_ref=src, dst_ref=dst, send_sem=send, recv_sem=recv, device_id={"dp": to}, device_id_type=MESH)

    barrier = pltpu.get_barrier_semaphore()
    for j in range(1, devices):
        pl.semaphore_signal(barrier, inc=1, device_id={"dp": lax.rem(me + j, devices)}, device_id_type=MESH)
    pl.semaphore_wait(barrier, devices - 1)

    x_at = []
    seen = [0, 0]
    for _, _, q in todo:
        kind = int(q[0] == 2)
        x_at.append((kind, seen[kind]))
        seen[kind] += 1
    xs, st_own, st_other, landed = (xw, xd), (ow, od), (pw, pd), (rw, rd)
    depth = [ow.shape[0], od.shape[0]]

    def target(way, d):
        return z if way is None else z + step[way] * d

    def exchange(i):
        way, d, q = todo[i]
        kind, k = x_at[i]
        return remote(term(q, at(target(way, d), 1 - c)), xs[kind].at[k], x_send.at[i], x_recv.at[i], partner)

    def stage(i):
        way, d, q = todo[i]
        kind, k = x_at[i]
        s = k % depth[kind]
        sem = kind * depth[0] + s
        return (
            pltpu.make_async_copy(term(q, at(target(way, d), c)), st_own[kind].at[s], st_sem.at[0, sem]),
            pltpu.make_async_copy(xs[kind].at[k], st_other[kind].at[s], st_sem.at[1, sem]),
        )

    def stage_start(i):
        exchange(i).wait_recv()
        for copy in stage(i):
            copy.start()

    def slices(kind, shape, size):
        if kind:
            r = max(16, size // shape[1])
            return shape[0] // r, lambda j: (pl.ds(pl.multiple_of(j * r, r), r), slice(None))
        cols = max(128, size // shape[0])
        return shape[1] // cols, lambda j: (slice(None), pl.ds(pl.multiple_of(j * cols, cols), cols))

    def added(dst, terms, kind, total=None):
        cuts, cut = slices(kind, dst.shape, 16384)

        def one(j, acc):
            part = cut(j)
            s = terms[0][part].astype(jnp.float32)
            for r in terms[1:]:
                s = s + r[part].astype(jnp.float32)
            s = s.astype(dst.dtype)
            dst[part] = s
            if acc is None:
                return None
            s = s.astype(jnp.float32)
            s = s * s
            s = jnp.sum(s.reshape(s.shape[0] // 8, 8, s.shape[1]), axis=0)
            for k in range(s.shape[1] // 128):
                acc = acc + s[:, k * 128 : (k + 1) * 128]
            return acc

        return lax.fori_loop(0, cuts, one, total)

    def ring(s):
        way, d, q = s
        kind, k = fresh[s] if s in fresh else arrives[(way, d + 1, q)]
        to_kind, to = arrives[s]
        i = items.index(s)
        return remote(landed[kind].at[k], landed[to_kind].at[to], rs_send.at[i], rs_recv.at[i], ahead[way])

    window = 12
    for i in range(window):
        exchange(i).start()
    reach = 2
    for i in range(reach):
        stage_start(i)

    def held(which, q):
        a, layer = q
        if a == 2:
            return mvd.at[which, layer]
        return mvw.at[which, a * layers + layer]

    def weight(q):
        a, layer = q
        return bd.at[layer] if a == 2 else bw.at[a * layers + layer]

    def fresh_weight(q):
        a, layer = q
        return wwd.at[layer] if a == 2 else ww.at[a * layers + layer]

    def load_state(e):
        q = pieces[e]
        a, layer = q
        return (
            pltpu.make_async_copy(m[a].at[layer], held(0, q), in_sem.at[0, e]),
            pltpu.make_async_copy(v[a].at[layer], held(1, q), in_sem.at[1, e]),
            pltpu.make_async_copy(block(w, q, me), weight(q), in_sem.at[2, e]),
        )

    total = jnp.zeros((8, 128), jnp.float32)
    for i, s in enumerate(todo):
        way, d, q = s
        kind, k = x_at[i]
        for copy in stage(i):
            copy.wait()
        terms = [st_own[kind].at[k % depth[kind]], st_other[kind].at[k % depth[kind]]]
        if way is not None:
            if s not in fresh:
                before = (way, d + 1, q)
                ring(before).wait_recv()
                ak, ai = arrives[before]
                terms.append(landed[ak].at[ai])
                dst = landed[ak].at[ai]
            else:
                fk, fi = fresh[s]
                dst = landed[fk].at[fi]
            added(dst, terms, kind)
            ring(s).start()
        else:
            for w_ in (PLUS, MINUS):
                ring((w_, 1, q)).wait_recv()
                ak, ai = arrives[(w_, 1, q)]
                terms.append(landed[ak].at[ai])
            total = added(fresh_weight(q), terms, kind, total)
        if i + window < len(todo):
            exchange(i + window).start()
        if i + reach < len(todo):
            stage_start(i + reach)
        if 8 <= i < 8 + len(pieces):
            for copy in load_state(i - 8):
                copy.start()

    squares[me] = total

    def share(j, sender):
        to = lax.rem(me + j, devices)
        return remote(squares.at[sender], squares.at[sender], sq_send.at[j - 1], sq_recv.at[j - 1], to)

    for j in range(1, devices):
        share(j, me).start()
    for i in range(len(todo)):
        exchange(i).wait_send()
    for s in items:
        ring(s).wait_send()
    for e in range(len(pieces)):
        for copy in load_state(e):
            copy.wait()
    for j in range(1, devices):
        share(j, lax.rem(me - j + devices, devices)).wait_recv()
    everyone = jnp.sum(jnp.sum(squares[...], axis=0), axis=(0, 1), keepdims=True)
    factor = jnp.minimum(1.0, 0.5 * lax.rsqrt(jnp.broadcast_to(everyone, (8, 128)) / count_all + 1e-30))[0:1, 0:1]

    def stepped(q):
        kind = int(q[0] == 2)
        wn, mr, vr, wr = fresh_weight(q), held(0, q), held(1, q), weight(q)
        cuts, cut = slices(kind, wn.shape, 8192)

        def one(j, _):
            part = cut(j)
            grad = wn[part].astype(jnp.float32) * factor
            mm = 0.9 * mr[part] + 0.1 * grad
            vv = 0.95 * vr[part] + 0.05 * grad * grad
            mr[part] = mm
            vr[part] = vv
            old = wr[part].astype(jnp.float32)
            wn[part] = (old - 0.02 * (mm * lax.rsqrt(vv + 1e-8) + 0.1 * old)).astype(wn.dtype)
            return None

        lax.fori_loop(0, cuts, one, None)

    order = [q for q in pieces if q[1] % 2] + [q for q in pieces if not q[1] % 2]
    gathers = [(way, h, q) for h in range(1, half) for q in order for way in (PLUS, MINUS)]

    def lies(way, h, q, owner):
        if h == half - 1 and q in last_hop(way, layers):
            kind, k = last_slot(way, layers, q)
            return last[way][kind].at[k]
        return block(t, q, owner)

    def pass_on(s, arriving):
        way, h, q = s
        owner = at(z - step[way] * (h if arriving else h - 1), c)
        i = gathers.index(s)
        src = fresh_weight(q) if h == 1 and not arriving else block(t, q, owner)
        return remote(src, lies(way, h, q, owner), ag_send.at[i], ag_recv.at[i], ahead[way])

    def across(i, arriving):
        core = 1 - c if arriving else c
        if i < len(gathers):
            way, h, q = gathers[i]
            owner = at(z - step[way] * h, core)
            src = lies(way, h, q, owner)
        else:
            q = order[i - len(gathers)]
            owner = at(z, core)
            src = block(t, q, owner) if arriving else fresh_weight(q)
        return remote(src, block(t, q, owner), y_send.at[i], y_recv.at[i], partner)

    def results(e):
        q = pieces[e]
        a, layer = q
        return (
            pltpu.make_async_copy(held(0, q), om[a].at[layer], out_sem.at[0, e]),
            pltpu.make_async_copy(held(1, q), ov[a].at[layer], out_sem.at[1, e]),
            pltpu.make_async_copy(fresh_weight(q), block(t, q, me), out_sem.at[2, e]),
        )

    for q in order:
        stepped(q)
        for way in (PLUS, MINUS):
            pass_on((way, 1, q), False).start()
        across(len(gathers) + order.index(q), False).start()
        for copy in results(pieces.index(q)):
            copy.start()
    for i, s in enumerate(gathers):
        way, h, q = s
        pass_on(s, True).wait_recv()
        if (way, h + 1, q) in gathers:
            pass_on((way, h + 1, q), False).start()
        across(i, False).start()
    for j in range(1, devices):
        share(j, me).wait_send()
    for e in range(len(pieces)):
        for copy in results(e):
            copy.wait()
    for s in gathers:
        pass_on(s, False).wait_send()
    for i in range(len(gathers) + len(order)):
        across(i, False).wait_send()
    for i in range(len(gathers) + len(order)):
        across(i, True).wait_recv()


def moved(jobs, sem):
    ins = [pltpu.make_async_copy(a, b, sem.at[0, j]) for j, (a, b, _) in enumerate(jobs)]
    outs = [pltpu.make_async_copy(b, c, sem.at[1, j]) for j, (_, b, c) in enumerate(jobs)]
    for copy in ins:
        copy.start()
    for copy, then in zip(ins, outs, strict=True):
        copy.wait()
        then.start()
    for copy in outs:
        copy.wait()


def row_block(ref, layer, rows, owner):
    return ref.at[layer, pl.ds(pl.multiple_of(owner * rows, rows), rows)]


def settle(n, layers, arrays, rows, *refs):
    k = len(arrays)
    t, moments, last = refs[:k], refs[k : k + 3], {PLUS: refs[k + 3], MINUS: refs[k + 4]}
    outs, new = refs[k + 5 : 2 * k + 5], refs[2 * k + 5 : 2 * k + 8]
    buf, wide, down, sem = refs[2 * k + 8 :]
    half = n // 2
    me = lax.axis_index("dp")
    z, c = me // CORES, me % CORES
    jobs = []
    for off in range(n):
        if off == half:
            continue
        for core in (0, 1):
            owner = lax.rem(z + off, n) * CORES + (c if core == 0 else 1 - c)
            for j, a in enumerate(arrays):
                for layer in range(layers):
                    src = row_block(t[j], layer, rows, owner)
                    for way, far in ((PLUS, n - (half - 1)), (MINUS, half - 1)):
                        if core == 0 and off == far and (a, layer) in last_hop(way, layers):
                            src = last[way].at[last_slot(way, layers, (a, layer))[1]]
                    jobs.append((src, buf.at[len(jobs)], row_block(outs[j], layer, rows, owner)))
    for a in range(3):
        for layer in range(layers):
            via = down.at[layer] if a == 2 else wide.at[a * layers + layer]
            jobs.append((moments[a].at[layer], via, new[a].at[layer]))
    moved(jobs, sem)


def complete(n, layers, arrays, rows, *refs):
    k = len(arrays)
    came = {(way, core): refs[k + 2 * core + way] for core in (0, 1) for way in (PLUS, MINUS)}
    outs, sem = refs[k + 4 : 2 * k + 4], refs[2 * k + 4]
    me = lax.axis_index("dp")
    z, c = me // CORES, me % CORES
    copies = []
    for (way, core), ref in came.items():
        owner = lax.rem(z + n // 2, n) * CORES + (c if core == 0 else 1 - c)
        for a, layer in last_hop(way, layers):
            if a in arrays:
                src = ref.at[last_slot(way, layers, (a, layer))[1]]
                copies.append(pltpu.make_async_copy(src, row_block(outs[arrays.index(a)], layer, rows, owner), sem.at[len(copies)]))
    for copy in copies:
        copy.start()
    for copy in copies:
        copy.wait()


def solution(mesh):
    devices = mesh.shape["dp"]
    n = devices // CORES
    hbm = pl.BlockSpec(memory_space=pl.ANY)
    bf, f32 = jnp.bfloat16, jnp.float32
    dma = pltpu.SemaphoreType.DMA
    like = lambda a: jax.ShapeDtypeStruct(a.shape, a.dtype)
    limit = pltpu.CompilerParams(vmem_limit_bytes=60 * 2**20)

    def summed(terms, weights, m, v):
        layers = m[0].shape[0]
        items, finals, _, _, count = plan(n, layers)
        todo = items + finals
        wide, down = m[0].shape[1:], m[2].shape[1:]
        n_down = sum(q[0] == 2 for _, _, q in todo)
        sizes = devices * sum(one.size for one in m)
        pieces = len(pieces_of(layers))
        gathers = 2 * (n // 2 - 1) * pieces
        lasts = []
        for way in (PLUS, MINUS):
            qs = last_hop(way, layers)
            lasts.append(jax.ShapeDtypeStruct((sum(q[0] < 2 for q in qs), *wide), bf))
            lasts.append(jax.ShapeDtypeStruct((sum(q[0] == 2 for q in qs), *down), bf))
        return pl.pallas_call(
            functools.partial(kernel, n, sizes),
            out_shape=[like(w) for w in weights]
            + [like(one) for one in (*m, *v)]
            + [jax.ShapeDtypeStruct((len(todo) - n_down, *wide), bf), jax.ShapeDtypeStruct((n_down, *down), bf)]
            + lasts,
            in_specs=[hbm] * 12,
            out_specs=[hbm] * 15,
            scratch_shapes=[
                pltpu.VMEM((count[0], *wide), bf),
                pltpu.VMEM((count[1], *down), bf),
                pltpu.VMEM((4, *wide), bf),
                pltpu.VMEM((2, *down), bf),
                pltpu.VMEM((4, *wide), bf),
                pltpu.VMEM((2, *down), bf),
                pltpu.VMEM((2, 2 * layers, *wide), f32),
                pltpu.VMEM((2, layers, *down), f32),
                pltpu.VMEM((2 * layers, *wide), bf),
                pltpu.VMEM((layers, *down), bf),
                pltpu.VMEM((2 * layers, *wide), bf),
                pltpu.VMEM((layers, *down), bf),
                pltpu.VMEM((devices, 8, 128), f32),
                dma((len(items),)),
                dma((len(items),)),
                dma((len(todo),)),
                dma((len(todo),)),
                dma((2, 6)),
                dma((gathers,)),
                dma((gathers,)),
                dma((gathers + pieces,)),
                dma((gathers + pieces,)),
                dma((devices - 1,)),
                dma((devices - 1,)),
                dma((3, pieces)),
                dma((3, pieces)),
            ],
            compiler_params=pltpu.CompilerParams(collective_id=0, has_side_effects=True, vmem_limit_bytes=60 * 2**20),
            name="summed",
        )(*terms, *weights, *m, *v)

    def settled(arrays, t, moments, last):
        layers, rows = moments[0].shape[0], moments[arrays[0]].shape[1]
        jobs = CORES * (n - 1) * len(arrays) * layers
        moved_bytes = 2 * (jobs * rows * t[0].shape[2] * 2 + 4 * sum(one.size for one in moments))
        return pl.pallas_call(
            functools.partial(settle, n, layers, arrays, rows),
            out_shape=[like(one) for one in (*t, *moments)],
            in_specs=[hbm] * (len(t) + 5),
            out_specs=[hbm] * (len(t) + 3),
            scratch_shapes=[
                pltpu.VMEM((jobs, rows, t[0].shape[2]), bf),
                pltpu.VMEM((2 * layers, *moments[0].shape[1:]), f32),
                pltpu.VMEM((layers, *moments[2].shape[1:]), f32),
                dma((2, jobs + 3 * layers)),
            ],
            compiler_params=limit,
            cost_estimate=pl.CostEstimate(flops=60 * moved_bytes, bytes_accessed=moved_bytes, transcendentals=0),
            name="settle",
        )(*t, *moments, *last)

    def completed(arrays, rows, results, came):
        layers = results[0].shape[0]
        jobs = CORES * len(arrays) * layers
        return pl.pallas_call(
            functools.partial(complete, n, layers, arrays, rows),
            out_shape=[like(one) for one in results],
            in_specs=[hbm] * len(results) + [pl.BlockSpec(memory_space=pltpu.VMEM)] * 4,
            out_specs=[hbm] * len(results),
            scratch_shapes=[dma((jobs,))],
            input_output_aliases={i: i for i in range(len(results))},
            compiler_params=pltpu.CompilerParams(vmem_limit_bytes=16 * 2**20),
            name="complete",
        )(*results, *came)

    def step(*arrays):
        terms, weights, m, v = (arrays[i : i + 3] for i in (0, 3, 6, 9))
        out = summed(terms, weights, m, v)
        t, new_m, new_v, last = out[:3], out[3:6], out[6:9], out[11:]
        onward = [(i, (i + CORES) % devices) for i in range(devices)]
        back = [(b, a) for a, b in onward]
        other = [(i, i + 1 - 2 * (i % CORES)) for i in range(devices)]

        def hop(k):
            return [lax.ppermute(last[k], "dp", onward), lax.ppermute(last[2 + k], "dp", back)]

        def cross(came):
            return [lax.ppermute(one, "dp", other) for one in came]

        rows = [one.shape[1] for one in m]
        wide = hop(0)
        down = hop(1)
        g, u, *m = settled((0, 1), t[:2], new_m, (last[0], last[2]))
        d, *v = settled((2,), t[2:], new_v, (last[1], last[3]))
        wide += cross(wide)
        down += cross(down)
        g, u = completed((0, 1), rows[0], (g, u), wide)
        (d,) = completed((2,), rows[2], (d,), down)
        return (g, u, d, *m, *v)

    all_of, cut = P(None, None, None), P(None, "dp", None)
    return jax.shard_map(
        step,
        mesh=mesh,
        in_specs=(P(("rep", "dp"), None, None, None),) * 3 + (all_of,) * 3 + (cut,) * 6,
        out_specs=(P("rep", None, None),) * 3 + (P("rep", "dp", None),) * 6,
        check_vma=False,
    )
```

```python
import functools

import jax
import jax.numpy as jnp
from jax import lax
from jax.experimental import pallas as pl
from jax.experimental.pallas import tpu as pltpu
from jax.sharding import PartitionSpec as P


MESH = pl.DeviceIdType.MESH
CORES = 2
PLUS, MINUS = WAYS = 0, 1
PARTS = 2
DOWN = 2


def pieces_of(layers):
    return [(a, layer, part) for part in range(PARTS) for layer in range(layers) for a in range(3)]


def kind_of(q):
    return int(q[0] == DOWN)


def place(q, among):
    return kind_of(q), [p for p in among if kind_of(p) == kind_of(q)].index(q)


def counts(among):
    return [sum(kind_of(q) == kind for q in among) for kind in (0, 1)]


def half_of(way, layers):
    return [q for q in pieces_of(layers) if q[2] % 2 == way]


def far_half(way, layers):
    return half_of(1 - way, layers)


def plan(n, layers):
    half = n // 2
    queue = {}
    for way in WAYS:
        mine, other = half_of(way, layers), half_of(1 - way, layers)
        sends = [(way, half, q) for q in mine]
        for d in range(half - 1, 0, -1):
            sends += [(way, d, q) for q in (other + mine if d > 1 else pieces_of(layers))]
        queue[way] = sends
    items = [s for pair in zip(queue[PLUS], queue[MINUS], strict=True) for s in pair]
    finals = [(None, 0, q) for q in pieces_of(layers)]
    arrives = {}
    fresh = {}
    count = [0, 0]

    def slot(q):
        count[kind_of(q)] += 1
        return kind_of(q), count[kind_of(q)] - 1

    for s in items:
        arrives[s] = slot(s[2])
    for s in items:
        if (s[0], s[1] + 1, s[2]) not in arrives:
            fresh[s] = slot(s[2])
    return items, finals, arrives, fresh, count


def kernel(n, count_all, *refs):
    g, w, m, v, t = (refs[i : i + 3] for i in range(0, 15, 3))
    xs, ms, vs, own_new = (refs[i : i + 2] for i in range(15, 23, 2))
    far = {way: refs[23 + 2 * way : 25 + 2 * way] for way in WAYS}
    near = {way: refs[27 + 2 * way : 29 + 2 * way] for way in WAYS}
    landed, st_own, st_other, old = (refs[i : i + 2] for i in range(31, 39, 2))
    squares, rs_send, rs_recv, x_send, x_recv, st_sem, ag_send, ag_recv, y_send, y_recv, sq_send, sq_recv, in_sem, _ = refs[39:]

    layers = m[0].shape[0]
    rows = [a.shape[1] for a in m]
    items, finals, arrives, fresh, _ = plan(n, layers)
    pieces = pieces_of(layers)
    todo = items + finals
    half = n // 2
    devices = n * CORES

    me = lax.axis_index("dp")
    z, c = me // CORES, me % CORES
    at = lambda chip, core: lax.rem(chip + n, n) * CORES + core
    partner = at(z, 1 - c)
    ahead = {PLUS: at(z + 1, c), MINUS: at(z - 1, c)}
    step = {PLUS: 1, MINUS: -1}

    def rows_of(q, owner):
        size = rows[q[0]] // PARTS
        return pl.ds(pl.multiple_of(owner * rows[q[0]] + q[2] * size, size), size)

    def block(ref, q, owner):
        return ref[q[0]].at[q[1], rows_of(q, owner)]

    def term(q, owner):
        return g[q[0]].at[0, q[1], rows_of(q, owner)]

    def kept(pair, q):
        kind, k = place(q, pieces)
        return pair[kind].at[k]

    def remote(src, dst, send, recv, to):
        return pltpu.make_async_remote_copy(src_ref=src, dst_ref=dst, send_sem=send, recv_sem=recv, device_id={"dp": to}, device_id_type=MESH)

    barrier = pltpu.get_barrier_semaphore()
    for to in (partner, ahead[PLUS], ahead[MINUS]):
        pl.semaphore_signal(barrier, inc=1, device_id={"dp": to}, device_id_type=MESH)
    pl.semaphore_wait(barrier, 3)

    x_at = []
    for _, _, q in todo:
        x_at.append((kind_of(q), sum(kind == kind_of(q) for kind, _ in x_at)))
    depth = [ref.shape[0] for ref in st_own]

    def target(way, d):
        return z if way is None else z + step[way] * d

    def exchange(i):
        way, d, q = todo[i]
        kind, k = x_at[i]
        return remote(term(q, at(target(way, d), 1 - c)), xs[kind].at[k], x_send.at[i], x_recv.at[i], partner)

    def stage(i):
        way, d, q = todo[i]
        kind, k = x_at[i]
        s = k % depth[kind]
        sem = kind * depth[0] + s
        return (
            pltpu.make_async_copy(term(q, at(target(way, d), c)), st_own[kind].at[s], st_sem.at[0, sem]),
            pltpu.make_async_copy(xs[kind].at[k], st_other[kind].at[s], st_sem.at[1, sem]),
        )

    def stage_start(i):
        exchange(i).wait_recv()
        for copy in stage(i):
            copy.start()

    def slices(kind, shape, size):
        if kind:
            r = max(16, size // shape[1])
            return shape[0] // r, lambda j: (pl.ds(pl.multiple_of(j * r, r), r), slice(None))
        cols = max(128, size // shape[0])
        return shape[1] // cols, lambda j: (slice(None), pl.ds(pl.multiple_of(j * cols, cols), cols))

    def added(dst, terms, kind, total=None):
        cuts, cut = slices(kind, dst.shape, 16384)

        def one(j, acc):
            part = cut(j)
            s = terms[0][part].astype(jnp.float32)
            for r in terms[1:]:
                s = s + r[part].astype(jnp.float32)
            s = s.astype(dst.dtype)
            dst[part] = s
            if acc is None:
                return None
            s = s.astype(jnp.float32)
            s = s * s
            s = jnp.sum(s.reshape(s.shape[0] // 8, 8, s.shape[1]), axis=0)
            for k in range(s.shape[1] // 128):
                acc = acc + s[:, k * 128 : (k + 1) * 128]
            return acc

        return lax.fori_loop(0, cuts, one, total)

    def ring(s):
        way, d, q = s
        kind, k = fresh[s] if s in fresh else arrives[(way, d + 1, q)]
        to_kind, to = arrives[s]
        i = items.index(s)
        return remote(landed[kind].at[k], landed[to_kind].at[to], rs_send.at[i], rs_recv.at[i], ahead[way])

    def load_state(e):
        q = pieces[e]
        part = (q[1], pl.ds(q[2] * (rows[q[0]] // PARTS), rows[q[0]] // PARTS))
        return (
            pltpu.make_async_copy(m[q[0]].at[part], kept(ms, q), in_sem.at[0, e]),
            pltpu.make_async_copy(v[q[0]].at[part], kept(vs, q), in_sem.at[1, e]),
            pltpu.make_async_copy(block(w, q, me), kept(old, q), in_sem.at[2, e]),
        )

    window, reach = 24, 3
    for i in range(window):
        exchange(i).start()
    for i in range(reach):
        stage_start(i)
    total = jnp.zeros((8, 128), jnp.float32)
    for i, s in enumerate(todo):
        way, d, q = s
        kind, k = x_at[i]
        for copy in stage(i):
            copy.wait()
        terms = [st_own[kind].at[k % depth[kind]], st_other[kind].at[k % depth[kind]]]
        if way is not None:
            if s not in fresh:
                ring((way, d + 1, q)).wait_recv()
                kind, k = arrives[(way, d + 1, q)]
                terms.append(landed[kind].at[k])
            else:
                kind, k = fresh[s]
            added(landed[kind].at[k], terms, kind)
            ring(s).start()
        else:
            for from_ in WAYS:
                ring((from_, 1, q)).wait_recv()
                kind, k = arrives[(from_, 1, q)]
                terms.append(landed[kind].at[k])
            total = added(kept(own_new, q), terms, kind, total)
        if i + window < len(todo):
            exchange(i + window).start()
        if i + reach < len(todo):
            stage_start(i + reach)
        if 12 <= i < 12 + len(pieces):
            for copy in load_state(i - 12):
                copy.start()

    squares[me] = total

    def share(j, sender):
        to = lax.rem(me + j, devices)
        return remote(squares.at[sender], squares.at[sender], sq_send.at[j - 1], sq_recv.at[j - 1], to)

    for j in range(1, devices):
        share(j, me).start()
    for i in range(len(todo)):
        exchange(i).wait_send()
    for s in items:
        ring(s).wait_send()
    for e in range(len(pieces)):
        for copy in load_state(e):
            copy.wait()
    for j in range(1, devices):
        share(j, lax.rem(me - j + devices, devices)).wait_recv()
    everyone = jnp.sum(jnp.sum(squares[...], axis=0), axis=(0, 1), keepdims=True)
    factor = jnp.minimum(1.0, 0.5 * lax.rsqrt(jnp.broadcast_to(everyone, (8, 128)) / count_all + 1e-30))[0:1, 0:1]

    def stepped(q):
        wn, mr, vr, wr = kept(own_new, q), kept(ms, q), kept(vs, q), kept(old, q)
        cuts, cut = slices(kind_of(q), wn.shape, 8192)

        def one(j, _):
            part = cut(j)
            grad = wn[part].astype(jnp.float32) * factor
            mm = 0.9 * mr[part] + 0.1 * grad
            vv = 0.95 * vr[part] + 0.05 * grad * grad
            mr[part] = mm
            vr[part] = vv
            before = wr[part].astype(jnp.float32)
            wn[part] = (before - 0.02 * (mm * lax.rsqrt(vv + 1e-8) + 0.1 * before)).astype(wn.dtype)
            return None

        lax.fori_loop(0, cuts, one, None)

    gathers = [(way, h, q) for h in range(1, half) for q in pieces for way in WAYS]

    def lies(way, h, q, owner):
        if h < half - 1:
            return block(t, q, owner)
        which, among = (far, far_half(way, layers)) if q in far_half(way, layers) else (near, half_of(way, layers))
        kind, k = place(q, among)
        return which[way][kind].at[k]

    def pass_on(s, arriving):
        way, h, q = s
        owner = at(z - step[way] * (h if arriving else h - 1), c)
        i = gathers.index(s)
        src = kept(own_new, q) if h == 1 and not arriving else block(t, q, owner)
        return remote(src, lies(way, h, q, owner), ag_send.at[i], ag_recv.at[i], ahead[way])

    def across(i, arriving):
        core = 1 - c if arriving else c
        if i < len(gathers):
            way, h, q = gathers[i]
            owner = at(z - step[way] * h, core)
            src = lies(way, h, q, owner)
        else:
            q = pieces[i - len(gathers)]
            owner = at(z, core)
            src = kept(own_new, q)
        return remote(src, block(t, q, owner), y_send.at[i], y_recv.at[i], partner)

    for e, q in enumerate(pieces):
        stepped(q)
        for way in WAYS:
            pass_on((way, 1, q), False).start()
        across(len(gathers) + e, False).start()
    for i, s in enumerate(gathers):
        way, h, q = s
        pass_on(s, True).wait_recv()
        if h + 1 < half:
            pass_on((way, h + 1, q), False).start()
        across(i, False).start()
    for j in range(1, devices):
        share(j, me).wait_send()
    for s in gathers:
        pass_on(s, False).wait_send()
    for i in range(len(gathers) + len(pieces)):
        across(i, False).wait_send()
    for i in range(len(gathers) + len(pieces)):
        across(i, True).wait_recv()


def moved(jobs, sem):
    ins = [pltpu.make_async_copy(a, b, sem.at[0, j]) if b is not None else None for j, (a, b, _) in enumerate(jobs)]
    outs = [pltpu.make_async_copy(a if b is None else b, c, sem.at[1, j]) for j, (a, b, c) in enumerate(jobs)]
    for copy in ins:
        if copy is not None:
            copy.start()
    for copy, then in zip(ins, outs, strict=True):
        if copy is None:
            then.start()
    for copy, then in zip(ins, outs, strict=True):
        if copy is not None:
            copy.wait()
            then.start()
    for copy in outs:
        copy.wait()


def row_part(ref, layer, part, rows, owner):
    size = rows // PARTS
    return ref.at[layer, pl.ds(pl.multiple_of(owner * rows + part * size, size), size)]


def moment_jobs(pair, results, layers):
    pieces = pieces_of(layers)
    jobs = []
    for q in pieces:
        a, layer, part = q
        kind, k = place(q, pieces)
        size = results[a].shape[1] // PARTS
        jobs.append((pair[kind].at[k], None, results[a].at[layer, pl.ds(part * size, size)]))
    return jobs


def settle(n, layers, arrays, rows, moment, *refs):
    k = len(arrays)
    t, own, refs = refs[:k], refs[k], refs[k + 1 :]
    far, near, refs = refs[0:2], refs[2:4], refs[4:]
    pair, refs = (refs[:2], refs[2:]) if moment else (None, refs)
    outs, refs = refs[:k], refs[k:]
    results, refs = (refs[:3], refs[3:]) if moment else (None, refs)
    buf, sem = refs
    half = n // 2
    me = lax.axis_index("dp")
    z, c = me // CORES, me % CORES
    pieces = pieces_of(layers)
    jobs = moment_jobs(pair, results, layers) if moment else []
    through = 0
    for off in range(n):
        if off == half:
            continue
        for core in range(CORES):
            owner = lax.rem(z + off, n) * CORES + (c if core == 0 else 1 - c)
            for q in pieces:
                a, layer, part = q
                if a not in arrays:
                    continue
                dst = row_part(outs[arrays.index(a)], layer, part, rows, owner)
                src = None
                if core == 0 and off == 0:
                    src = own.at[place(q, pieces)[1]]
                for way, come in ((PLUS, n - (half - 1)), (MINUS, half - 1)):
                    if core == 0 and off == come:
                        which, among = (far, far_half(way, layers)) if q in far_half(way, layers) else (near, half_of(way, layers))
                        src = which[way].at[place(q, among)[1]]
                if src is not None:
                    jobs.append((src, None, dst))
                else:
                    jobs.append((row_part(t[arrays.index(a)], layer, part, rows, owner), buf.at[through], dst))
                    through += 1
    moved(jobs, sem)


def settle_moment(layers, *refs):
    moved(moment_jobs(refs[:2], refs[2:5], layers), refs[5])


def complete(n, layers, rows, *refs):
    came, outs, sem = refs[3:11], refs[11:14], refs[14]
    me = lax.axis_index("dp")
    z, c = me // CORES, me % CORES
    jobs = []
    for core in range(CORES):
        owner = lax.rem(z + n // 2, n) * CORES + (c if core == 0 else 1 - c)
        for way in WAYS:
            for q in far_half(way, layers):
                kind, k = place(q, far_half(way, layers))
                jobs.append((came[4 * kind + 2 * core + way].at[k], None, row_part(outs[q[0]], q[1], q[2], rows[q[0]], owner)))
    moved(jobs, sem)


def solution(mesh):
    devices = mesh.shape["dp"]
    n = devices // CORES
    hbm, vmem = pl.BlockSpec(memory_space=pltpu.HBM), pl.BlockSpec(memory_space=pltpu.VMEM)
    bf, f32 = jnp.bfloat16, jnp.float32
    dma = pltpu.SemaphoreType.DMA
    like = lambda a: jax.ShapeDtypeStruct(a.shape, a.dtype)

    def params(mib, **more):
        return pltpu.CompilerParams(vmem_limit_bytes=mib * 2**20, **more)

    def summed(terms, weights, m, v):
        layers = m[0].shape[0]
        items, finals, _, _, count = plan(n, layers)
        pieces = pieces_of(layers)
        todo = items + finals
        shapes = [(m[a].shape[1] // PARTS, m[a].shape[2]) for a in (0, DOWN)]
        pair = lambda make, number, dtype: [make((number[kind], *shapes[kind]), dtype) for kind in (0, 1)]
        whole, part = counts(pieces), counts(half_of(PLUS, layers))
        hops = 2 * (n // 2 - 1) * len(pieces)
        outs = [like(w) for w in weights] + pair(jax.ShapeDtypeStruct, counts([s[2] for s in todo]), bf)
        held = 2 * pair(pltpu.VMEM, whole, f32) + pair(pltpu.VMEM, whole, bf) + 4 * pair(pltpu.VMEM, part, bf)
        return pl.pallas_call(
            functools.partial(kernel, n, devices * sum(one.size for one in m)),
            out_shape=outs + held,
            in_specs=[hbm] * 12,
            out_specs=[hbm] * len(outs) + [vmem] * len(held),
            scratch_shapes=pair(pltpu.VMEM, count, bf)
            + 2 * pair(pltpu.VMEM, (4, 2), bf)
            + pair(pltpu.VMEM, whole, bf)
            + [pltpu.VMEM((devices, 8, 128), f32)]
            + [dma((len(items),))] * 2
            + [dma((len(todo),))] * 2
            + [dma((2, 6))]
            + [dma((hops,))] * 2
            + [dma((hops + len(pieces),))] * 2
            + [dma((devices - 1,))] * 2
            + [dma((3, len(pieces)))] * 2,
            compiler_params=params(38, collective_id=0, has_side_effects=True),
            name="summed",
        )(*terms, *weights, *m, *v)

    def settled(arrays, t, own, far, near, m, moment=()):
        layers, rows = m[0].shape[0], m[arrays[0]].shape[1]
        through = ((n - 1) * CORES - 3) * len(arrays) * layers * PARTS
        jobs = (n - 1) * CORES * len(arrays) * layers * PARTS + (len(pieces_of(layers)) if moment else 0)
        size = rows // PARTS * t[0].shape[2]
        moved_bytes = 2 * size * (jobs + through)
        results = [like(one) for one in m] if moment else []
        return pl.pallas_call(
            functools.partial(settle, n, layers, arrays, rows, bool(moment)),
            out_shape=[like(one) for one in t] + results,
            in_specs=[hbm] * len(t) + [vmem] * (5 + len(moment)),
            out_specs=[hbm] * (len(t) + len(results)),
            scratch_shapes=[pltpu.VMEM((through, rows // PARTS, t[0].shape[2]), bf), dma((2, jobs))],
            compiler_params=params(2 * size * through // 2**20 + 2),
            cost_estimate=pl.CostEstimate(flops=60 * moved_bytes, bytes_accessed=moved_bytes, transcendentals=0),
            name="settle",
        )(*(pltpu.with_memory_space_constraint(one, pltpu.HBM) for one in t), own, *far, *near, *moment)

    def settled_moment(m, moment):
        layers = m[0].shape[0]
        size = 4 * sum(one.size for one in m)
        return pl.pallas_call(
            functools.partial(settle_moment, layers),
            out_shape=[like(one) for one in m],
            in_specs=[vmem] * 2,
            out_specs=[hbm] * 3,
            scratch_shapes=[dma((2, len(pieces_of(layers))))],
            compiler_params=params(16),
            cost_estimate=pl.CostEstimate(flops=60 * size, bytes_accessed=size, transcendentals=0),
            name="settle_moment",
        )(*moment)

    def completed(results, came, rows):
        layers = results[0].shape[0]
        return pl.pallas_call(
            functools.partial(complete, n, layers, rows),
            out_shape=[like(one) for one in results],
            in_specs=[hbm] * 3 + [vmem] * 8,
            out_specs=[hbm] * 3,
            scratch_shapes=[dma((2, CORES * len(pieces_of(layers))))],
            input_output_aliases={i: i for i in range(3)},
            compiler_params=params(16),
            name="complete",
        )(*results, *came)

    def step(*arrays):
        terms, weights, m, v = (arrays[i : i + 3] for i in (0, 3, 6, 9))
        out = summed(terms, weights, m, v)
        t = out[:3]
        new_m, new_v, own = (out[i : i + 2] for i in (5, 7, 9))
        far, near = (out[11], out[13], out[12], out[14]), (out[15], out[17], out[16], out[18])
        onward = [(i, (i + CORES) % devices) for i in range(devices)]
        back = [(b, a) for a, b in onward]
        other = [(i, i + 1 - 2 * (i % CORES)) for i in range(devices)]

        def hop(k):
            return [lax.ppermute(one, "dp", way) for one, way in zip(far[k : k + 2], (onward, back), strict=True)]

        def cross(came):
            return came + [lax.ppermute(one, "dp", other) for one in came]

        wide = hop(0)
        down = hop(2)
        new_g, new_u, *ms = settled((0, 1), t[:2], own[0], far[:2], near[:2], m, new_m)
        (new_d,) = settled((2,), t[2:], own[1], far[2:], near[2:], m)
        vs = settled_moment(v, new_v)
        wide = cross(wide)
        down = cross(down)
        whole = completed((new_g, new_u, new_d), wide + down, [one.shape[1] for one in m])
        return (*whole, *ms, *vs)

    all_of, cut = P(None, None, None), P(None, "dp", None)
    return jax.shard_map(
        step,
        mesh=mesh,
        in_specs=(P(("rep", "dp"), None, None, None),) * 3 + (all_of,) * 3 + (cut,) * 6,
        out_specs=(P("rep", None, None),) * 3 + (P("rep", "dp", None),) * 6,
        check_vma=False,
    )
```

```python
import functools

import jax
import jax.numpy as jnp
from jax import lax
from jax.experimental import pallas as pl
from jax.experimental.pallas import tpu as pltpu
from jax.sharding import PartitionSpec as P


MESH = pl.DeviceIdType.MESH
CORES = 2
PLUS, MINUS = WAYS = 0, 1
PARTS = 2
DOWN = 2


def pieces_of(layers):
    return [(a, layer, part) for part in range(PARTS) for layer in range(layers) for a in range(3)]


def kind_of(q):
    return int(q[0] == DOWN)


def place(q, among):
    return kind_of(q), [p for p in among if kind_of(p) == kind_of(q)].index(q)


def counts(among):
    return [sum(kind_of(q) == kind for q in among) for kind in (0, 1)]


def half_of(way, layers):
    return [q for q in pieces_of(layers) if q[2] % 2 == way]


def far_half(way, layers):
    return half_of(1 - way, layers)


def plan(n, layers):
    half = n // 2
    queue = {}
    for way in WAYS:
        mine, other = half_of(way, layers), half_of(1 - way, layers)
        sends = [(way, half, q) for q in mine]
        for d in range(half - 1, 0, -1):
            sends += [(way, d, q) for q in (other + mine if d > 1 else pieces_of(layers))]
        queue[way] = sends
    items = [s for pair in zip(queue[PLUS], queue[MINUS], strict=True) for s in pair]
    finals = [(None, 0, q) for q in pieces_of(layers)]
    arrives = {}
    fresh = {}
    count = [0, 0]

    def slot(q):
        count[kind_of(q)] += 1
        return kind_of(q), count[kind_of(q)] - 1

    for s in items:
        arrives[s] = slot(s[2])
    for s in items:
        if (s[0], s[1] + 1, s[2]) not in arrives:
            fresh[s] = slot(s[2])
    return items, finals, arrives, fresh, count


def grouped(number, size, alone):
    of, lengths = [], []
    for k in range(number):
        if k < number - alone and k % size:
            lengths[-1] += 1
        else:
            lengths.append(1)
        of.append(len(lengths) - 1)
    return of, lengths


def groups_of(n, layers):
    items, finals, _, _, _ = plan(n, layers)
    pieces = len(pieces_of(layers))
    ring = grouped(len(items) // 2, 3, 3)
    of, lengths = grouped(len(items) + len(finals), 6, 6)
    terms = [len(lengths) - 1 - k for k in reversed(of)], lengths[::-1]
    return ring, terms, grouped((n // 2 - 1) * pieces, 3, 3)


def waited(ref, sem):
    pltpu.make_async_copy(ref, ref, sem).wait()


def kernel(n, count_all, *refs):
    g, w, m, v, t = (refs[i : i + 3] for i in range(0, 15, 3))
    xs, ms, vs, own_new = (refs[i : i + 2] for i in range(15, 23, 2))
    far = {way: refs[23 + 2 * way : 25 + 2 * way] for way in WAYS}
    near = {way: refs[27 + 2 * way : 29 + 2 * way] for way in WAYS}
    landed, st_own, st_other, old = (refs[i : i + 2] for i in range(31, 39, 2))
    squares, rs_send, rs_recv, x_send, x_recv, st_sem, ag_send, ag_recv, y_send, y_recv, sq_send, sq_recv, in_sem = refs[39:]

    layers = m[0].shape[0]
    rows = [a.shape[1] for a in m]
    items, finals, arrives, fresh, _ = plan(n, layers)
    pieces = pieces_of(layers)
    todo = items + finals
    half = n // 2
    devices = n * CORES
    ring_groups, term_groups, gather_groups = groups_of(n, layers)
    met = set()

    def arrive(name, sem, groups, way, k):
        of, lengths = groups
        if (name, way, of[k]) not in met:
            met.add((name, way, of[k]))
            waited(landed[0].at[pl.ds(0, lengths[of[k]])], sem.at[way * len(lengths) + of[k]])

    me = lax.axis_index("dp")
    z, c = me // CORES, me % CORES
    at = lambda chip, core: lax.rem(chip + n, n) * CORES + core
    partner = at(z, 1 - c)
    ahead = {PLUS: at(z + 1, c), MINUS: at(z - 1, c)}
    step = {PLUS: 1, MINUS: -1}

    def rows_of(q, owner):
        size = rows[q[0]] // PARTS
        return pl.ds(pl.multiple_of(owner * rows[q[0]] + q[2] * size, size), size)

    def block(ref, q, owner):
        return ref[q[0]].at[q[1], rows_of(q, owner)]

    def term(q, owner):
        return g[q[0]].at[0, q[1], rows_of(q, owner)]

    def kept(pair, q):
        kind, k = place(q, pieces)
        return pair[kind].at[k]

    def remote(src, dst, send, recv, to):
        return pltpu.make_async_remote_copy(src_ref=src, dst_ref=dst, send_sem=send, recv_sem=recv, device_id={"dp": to}, device_id_type=MESH)

    barrier = pltpu.get_barrier_semaphore()
    for to in (partner, ahead[PLUS], ahead[MINUS]):
        pl.semaphore_signal(barrier, inc=1, device_id={"dp": to}, device_id_type=MESH)
    pl.semaphore_wait(barrier, 3)

    x_at = []
    for _, _, q in todo:
        x_at.append((kind_of(q), sum(kind == kind_of(q) for kind, _ in x_at)))
    depth = [ref.shape[0] for ref in st_own]

    def target(way, d):
        return z if way is None else z + step[way] * d

    def exchange(i):
        way, d, q = todo[i]
        kind, k = x_at[i]
        return remote(term(q, at(target(way, d), 1 - c)), xs[kind].at[k], x_send.at[kind], x_recv.at[term_groups[0][i]], partner)

    def stage(i):
        way, d, q = todo[i]
        kind, k = x_at[i]
        s = k % depth[kind]
        sem = kind * depth[0] + s
        return (
            pltpu.make_async_copy(term(q, at(target(way, d), c)), st_own[kind].at[s], st_sem.at[0, sem]),
            pltpu.make_async_copy(xs[kind].at[k], st_other[kind].at[s], st_sem.at[1, sem]),
        )

    def stage_start(i):
        arrive("term", x_recv, term_groups, 0, i)
        for copy in stage(i):
            copy.start()

    def slices(kind, shape, size):
        if kind:
            r = max(16, size // shape[1])
            return shape[0] // r, lambda j: (pl.ds(pl.multiple_of(j * r, r), r), slice(None))
        cols = max(128, size // shape[0])
        return shape[1] // cols, lambda j: (slice(None), pl.ds(pl.multiple_of(j * cols, cols), cols))

    def added(dst, terms, kind, total=None):
        cuts, cut = slices(kind, dst.shape, 16384)

        def one(j, acc):
            part = cut(j)
            s = terms[0][part].astype(jnp.float32)
            for r in terms[1:]:
                s = s + r[part].astype(jnp.float32)
            s = s.astype(dst.dtype)
            dst[part] = s
            if acc is None:
                return None
            s = s.astype(jnp.float32)
            s = s * s
            s = jnp.sum(s.reshape(s.shape[0] // 8, 8, s.shape[1]), axis=0)
            for k in range(s.shape[1] // 128):
                acc = acc + s[:, k * 128 : (k + 1) * 128]
            return acc

        return lax.fori_loop(0, cuts, one, total)

    def ring(s):
        way, d, q = s
        kind, k = fresh[s] if s in fresh else arrives[(way, d + 1, q)]
        to_kind, to = arrives[s]
        group = way * len(ring_groups[1]) + ring_groups[0][items.index(s) // 2]
        return remote(landed[kind].at[k], landed[to_kind].at[to], rs_send.at[kind], rs_recv.at[group], ahead[way])

    def ring_arrive(s):
        arrive("ring", rs_recv, ring_groups, s[0], items.index(s) // 2)

    def load_state(e):
        q = pieces[e]
        part = (q[1], pl.ds(q[2] * (rows[q[0]] // PARTS), rows[q[0]] // PARTS))
        return (
            pltpu.make_async_copy(m[q[0]].at[part], kept(ms, q), in_sem.at[0, kind_of(q)]),
            pltpu.make_async_copy(v[q[0]].at[part], kept(vs, q), in_sem.at[1, kind_of(q)]),
            pltpu.make_async_copy(block(w, q, me), kept(old, q), in_sem.at[2, kind_of(q)]),
        )

    window, reach = 24, 3
    for i in range(window):
        exchange(i).start()
    for i in range(reach):
        stage_start(i)
    total = jnp.zeros((8, 128), jnp.float32)
    for i, s in enumerate(todo):
        way, d, q = s
        kind, k = x_at[i]
        for copy in stage(i):
            copy.wait()
        terms = [st_own[kind].at[k % depth[kind]], st_other[kind].at[k % depth[kind]]]
        if way is not None:
            if s not in fresh:
                ring_arrive((way, d + 1, q))
                kind, k = arrives[(way, d + 1, q)]
                terms.append(landed[kind].at[k])
            else:
                kind, k = fresh[s]
            added(landed[kind].at[k], terms, kind)
            ring(s).start()
        else:
            for from_ in WAYS:
                ring_arrive((from_, 1, q))
                kind, k = arrives[(from_, 1, q)]
                terms.append(landed[kind].at[k])
            total = added(kept(own_new, q), terms, kind, total)
        if i + window < len(todo):
            exchange(i + window).start()
        if i + reach < len(todo):
            stage_start(i + reach)
        if 12 <= i < 12 + len(pieces):
            for copy in load_state(i - 12):
                copy.start()

    squares[me] = total

    def share(j):
        return remote(squares.at[me], squares.at[me], sq_send.at[0], sq_recv.at[0], lax.rem(me + j, devices))

    def several(number, ref):
        return ref.at[pl.ds(0, number)]

    for j in range(1, devices):
        share(j).start()
    for kind in (0, 1):
        waited(xs[kind], x_send.at[kind])
        waited(several(sum(kind_of(s[2]) == kind for s in items), landed[kind]), rs_send.at[kind])
        for which, pair in enumerate((ms, vs, old)):
            waited(pair[kind], in_sem.at[which, kind])
    waited(several(devices - 1, squares), sq_recv.at[0])
    everyone = jnp.sum(jnp.sum(squares[...], axis=0), axis=(0, 1), keepdims=True)
    factor = jnp.minimum(1.0, 0.5 * lax.rsqrt(jnp.broadcast_to(everyone, (8, 128)) / count_all + 1e-30))[0:1, 0:1]

    def stepped(q):
        wn, mr, vr, wr = kept(own_new, q), kept(ms, q), kept(vs, q), kept(old, q)
        cuts, cut = slices(kind_of(q), wn.shape, 8192)

        def one(j, _):
            part = cut(j)
            grad = wn[part].astype(jnp.float32) * factor
            mm = 0.9 * mr[part] + 0.1 * grad
            vv = 0.95 * vr[part] + 0.05 * grad * grad
            mr[part] = mm
            vr[part] = vv
            before = wr[part].astype(jnp.float32)
            wn[part] = (before - 0.02 * (mm * lax.rsqrt(vv + 1e-8) + 0.1 * before)).astype(wn.dtype)
            return None

        lax.fori_loop(0, cuts, one, None)

    gathers = [(way, h, q) for h in range(1, half) for q in pieces for way in WAYS]

    def lies(way, h, q, owner):
        if h < half - 1:
            return block(t, q, owner)
        which, among = (far, far_half(way, layers)) if q in far_half(way, layers) else (near, half_of(way, layers))
        kind, k = place(q, among)
        return which[way][kind].at[k]

    def pass_on(s):
        way, h, q = s
        owner = at(z - step[way] * (h - 1), c)
        group = way * len(gather_groups[1]) + gather_groups[0][gathers.index(s) // 2]
        src = kept(own_new, q) if h == 1 else block(t, q, owner)
        return remote(src, lies(way, h, q, owner), ag_send.at[kind_of(q)], ag_recv.at[group], ahead[way])

    def across(q, owner, src):
        return remote(src, block(t, q, owner), y_send.at[kind_of(q)], y_recv.at[kind_of(q)], partner)

    for q in pieces:
        stepped(q)
        for way in WAYS:
            pass_on((way, 1, q)).start()
        across(q, me, kept(own_new, q)).start()
    for i, s in enumerate(gathers):
        way, h, q = s
        owner = at(z - step[way] * h, c)
        arrive("gather", ag_recv, gather_groups, way, i // 2)
        if h + 1 < half:
            pass_on((way, h + 1, q)).start()
        across(q, owner, lies(way, h, q, owner)).start()
    waited(several(devices - 1, squares), sq_send.at[0])
    for kind in (0, 1):
        number = sum(kind_of(s[2]) == kind for s in gathers)
        waited(several(number, landed[kind]), ag_send.at[kind])
        number += sum(kind_of(q) == kind for q in pieces)
        waited(several(number, landed[kind]), y_send.at[kind])
        waited(several(number, landed[kind]), y_recv.at[kind])


READS = 4


def moved(sem, through=(), buf=None, direct=()):
    reads = -(-len(through) // READS)
    for j, (a, _) in enumerate(through):
        pltpu.make_async_copy(a, buf.at[j], sem.at[j // READS]).start()
    for k, (copies, _) in enumerate(direct):
        for a, b in copies:
            pltpu.make_async_copy(a, b, sem.at[reads + 1 + k]).start()
    for i in range(reads):
        these = range(i * READS, min(len(through), (i + 1) * READS))
        waited(buf.at[pl.ds(i * READS, len(these))], sem.at[i])
        for j in these:
            pltpu.make_async_copy(buf.at[j], through[j][1], sem.at[reads]).start()
    if through:
        waited(buf, sem.at[reads])
    for k, (_, total) in enumerate(direct):
        waited(total, sem.at[reads + 1 + k])


def row_part(ref, layer, part, rows, owner):
    size = rows // PARTS
    return ref.at[layer, pl.ds(pl.multiple_of(owner * rows + part * size, size), size)]


def moment_copies(pair, results, layers):
    pieces = pieces_of(layers)
    sets = [([], pair[0]), ([], pair[1])]
    for q in pieces:
        a, layer, part = q
        kind, k = place(q, pieces)
        size = results[a].shape[1] // PARTS
        sets[kind][0].append((pair[kind].at[k], results[a].at[layer, pl.ds(part * size, size)]))
    return sets


def settle(n, layers, arrays, rows, moment, *refs):
    k = len(arrays)
    t, own, refs = refs[:k], refs[k], refs[k + 1 :]
    far, near, refs = refs[0:2], refs[2:4], refs[4:]
    pair, refs = (refs[:2], refs[2:]) if moment else (None, refs)
    outs, refs = refs[:k], refs[k:]
    results, refs = (refs[:3], refs[3:]) if moment else (None, refs)
    buf, sem = refs
    half = n // 2
    me = lax.axis_index("dp")
    z, c = me // CORES, me % CORES
    pieces = pieces_of(layers)
    through, held = [], []
    for off in range(n):
        if off == half:
            continue
        for core in range(CORES):
            owner = lax.rem(z + off, n) * CORES + (c if core == 0 else 1 - c)
            for q in pieces:
                a, layer, part = q
                if a not in arrays:
                    continue
                dst = row_part(outs[arrays.index(a)], layer, part, rows, owner)
                src = None
                if core == 0 and off == 0:
                    src = own.at[place(q, pieces)[1]]
                for way, come in ((PLUS, n - (half - 1)), (MINUS, half - 1)):
                    if core == 0 and off == come:
                        which, among = (far, far_half(way, layers)) if q in far_half(way, layers) else (near, half_of(way, layers))
                        src = which[way].at[place(q, among)[1]]
                if src is not None:
                    held.append((src, dst))
                else:
                    through.append((row_part(t[arrays.index(a)], layer, part, rows, owner), dst))
    direct = [(held, buf.at[pl.ds(0, len(held))])] + (moment_copies(pair, results, layers) if moment else [])
    moved(sem, through, buf, direct)


def settle_moment(layers, *refs):
    moved(refs[5], direct=moment_copies(refs[:2], refs[2:5], layers))


def complete(n, layers, rows, *refs):
    came, outs, sem = refs[3:11], refs[11:14], refs[14]
    me = lax.axis_index("dp")
    z, c = me // CORES, me % CORES
    copies = []
    for core in range(CORES):
        owner = lax.rem(z + n // 2, n) * CORES + (c if core == 0 else 1 - c)
        for way in WAYS:
            for q in far_half(way, layers):
                kind, k = place(q, far_half(way, layers))
                copies.append((came[4 * kind + 2 * core + way].at[k], row_part(outs[q[0]], q[1], q[2], rows[q[0]], owner)))
    moved(sem, direct=[(copies, outs[0].at[0, pl.ds(0, len(copies) * (rows[0] // PARTS))])])


def solution(mesh):
    devices = mesh.shape["dp"]
    n = devices // CORES
    hbm, vmem = pl.BlockSpec(memory_space=pltpu.HBM), pl.BlockSpec(memory_space=pltpu.VMEM)
    bf, f32 = jnp.bfloat16, jnp.float32
    dma = pltpu.SemaphoreType.DMA
    like = lambda a: jax.ShapeDtypeStruct(a.shape, a.dtype)

    def params(mib, **more):
        return pltpu.CompilerParams(vmem_limit_bytes=mib * 2**20, **more)

    def summed(terms, weights, m, v):
        layers = m[0].shape[0]
        items, finals, _, _, count = plan(n, layers)
        pieces = pieces_of(layers)
        todo = items + finals
        shapes = [(m[a].shape[1] // PARTS, m[a].shape[2]) for a in (0, DOWN)]
        pair = lambda make, number, dtype: [make((number[kind], *shapes[kind]), dtype) for kind in (0, 1)]
        whole, part = counts(pieces), counts(half_of(PLUS, layers))
        ring_groups, term_groups, gather_groups = groups_of(n, layers)
        outs = [like(w) for w in weights] + pair(jax.ShapeDtypeStruct, counts([s[2] for s in todo]), bf)
        held = 2 * pair(pltpu.VMEM, whole, f32) + pair(pltpu.VMEM, whole, bf) + 4 * pair(pltpu.VMEM, part, bf)
        return pl.pallas_call(
            functools.partial(kernel, n, devices * sum(one.size for one in m)),
            out_shape=outs + held,
            in_specs=[hbm] * 12,
            out_specs=[hbm] * len(outs) + [vmem] * len(held),
            scratch_shapes=pair(pltpu.VMEM, count, bf)
            + 2 * pair(pltpu.VMEM, (4, 2), bf)
            + pair(pltpu.VMEM, whole, bf)
            + [pltpu.VMEM((devices, 8, 128), f32)]
            + [dma((2,)), dma((2 * len(ring_groups[1]),))]
            + [dma((2,)), dma((len(term_groups[1]),))]
            + [dma((2, 6))]
            + [dma((2,)), dma((2 * len(gather_groups[1]),))]
            + [dma((2,)), dma((2,))]
            + [dma((1,)), dma((1,))]
            + [dma((3, 2))],
            compiler_params=params(38, collective_id=0, has_side_effects=True),
            name="summed",
        )(*terms, *weights, *m, *v)

    def settled(arrays, t, own, far, near, m, moment=()):
        layers, rows = m[0].shape[0], m[arrays[0]].shape[1]
        through = ((n - 1) * CORES - 3) * len(arrays) * layers * PARTS
        jobs = (n - 1) * CORES * len(arrays) * layers * PARTS + (len(pieces_of(layers)) if moment else 0)
        size = rows // PARTS * t[0].shape[2]
        moved_bytes = 2 * size * (jobs + through)
        results = [like(one) for one in m] if moment else []
        return pl.pallas_call(
            functools.partial(settle, n, layers, arrays, rows, bool(moment)),
            out_shape=[like(one) for one in t] + results,
            in_specs=[hbm] * len(t) + [vmem] * (5 + len(moment)),
            out_specs=[hbm] * (len(t) + len(results)),
            scratch_shapes=[pltpu.VMEM((through, rows // PARTS, t[0].shape[2]), bf), dma((-(-through // READS) + 4,))],
            compiler_params=params(2 * size * through // 2**20 + 2),
            cost_estimate=pl.CostEstimate(flops=60 * moved_bytes, bytes_accessed=moved_bytes, transcendentals=0),
            name="settle",
        )(*(pltpu.with_memory_space_constraint(one, pltpu.HBM) for one in t), own, *far, *near, *moment)

    def settled_moment(m, moment):
        layers = m[0].shape[0]
        size = 4 * sum(one.size for one in m)
        return pl.pallas_call(
            functools.partial(settle_moment, layers),
            out_shape=[like(one) for one in m],
            in_specs=[vmem] * 2,
            out_specs=[hbm] * 3,
            scratch_shapes=[dma((3,))],
            compiler_params=params(16),
            cost_estimate=pl.CostEstimate(flops=60 * size, bytes_accessed=size, transcendentals=0),
            name="settle_moment",
        )(*moment)

    def completed(results, came, rows):
        layers = results[0].shape[0]
        return pl.pallas_call(
            functools.partial(complete, n, layers, rows),
            out_shape=[like(one) for one in results],
            in_specs=[hbm] * 3 + [vmem] * 8,
            out_specs=[hbm] * 3,
            scratch_shapes=[dma((2,))],
            input_output_aliases={i: i for i in range(3)},
            compiler_params=params(16),
            name="complete",
        )(*results, *came)

    def step(*arrays):
        terms, weights, m, v = (arrays[i : i + 3] for i in (0, 3, 6, 9))
        out = summed(terms, weights, m, v)
        t = out[:3]
        new_m, new_v, own = (out[i : i + 2] for i in (5, 7, 9))
        far, near = (out[11], out[13], out[12], out[14]), (out[15], out[17], out[16], out[18])
        onward = [(i, (i + CORES) % devices) for i in range(devices)]
        back = [(b, a) for a, b in onward]
        other = [(i, i + 1 - 2 * (i % CORES)) for i in range(devices)]

        def hop(k):
            return [lax.ppermute(one, "dp", way) for one, way in zip(far[k : k + 2], (onward, back), strict=True)]

        def cross(came):
            return came + [lax.ppermute(one, "dp", other) for one in came]

        wide = hop(0)
        down = hop(2)
        new_g, new_u, *ms = settled((0, 1), t[:2], own[0], far[:2], near[:2], m, new_m)
        (new_d,) = settled((2,), t[2:], own[1], far[2:], near[2:], m)
        vs = settled_moment(v, new_v)
        wide = cross(wide)
        down = cross(down)
        whole = completed((new_g, new_u, new_d), wide + down, [one.shape[1] for one in m])
        return (*whole, *ms, *vs)

    all_of, cut = P(None, None, None), P(None, "dp", None)
    return jax.shard_map(
        step,
        mesh=mesh,
        in_specs=(P(("rep", "dp"), None, None, None),) * 3 + (all_of,) * 3 + (cut,) * 6,
        out_specs=(P("rep", None, None),) * 3 + (P("rep", "dp", None),) * 6,
        check_vma=False,
    )
```

```python
import functools

import jax
import jax.numpy as jnp
from jax import lax
from jax.experimental import pallas as pl
from jax.experimental.pallas import tpu as pltpu
from jax.sharding import PartitionSpec as P


MESH = pl.DeviceIdType.MESH
CORES = 2
PLUS, MINUS = WAYS = 0, 1
PARTS = 2
DOWN = 2


def pieces_of(layers):
    return [(a, layer, part) for part in range(PARTS) for layer in range(layers) for a in range(3)]


def kind_of(q):
    return int(q[0] == DOWN)


def place(q, among):
    return kind_of(q), [p for p in among if kind_of(p) == kind_of(q)].index(q)


def counts(among):
    return [sum(kind_of(q) == kind for q in among) for kind in (0, 1)]


def half_of(way, layers):
    return [q for q in pieces_of(layers) if q[2] % 2 == way]


def far_half(way, layers):
    return half_of(1 - way, layers)


def late(n, way, h, q):
    return h == n // 2 - 1 and q[0] == DOWN and q[2] == PARTS - 1


def plan(n, layers):
    half = n // 2
    queue = {}
    for way in WAYS:
        mine, other = half_of(way, layers), half_of(1 - way, layers)
        sends = [(way, half, q) for q in mine]
        for d in range(half - 1, 0, -1):
            sends += [(way, d, q) for q in (other + mine if d > 1 else pieces_of(layers))]
        queue[way] = sends
    items = [s for pair in zip(queue[PLUS], queue[MINUS], strict=True) for s in pair]
    finals = [(None, 0, q) for q in pieces_of(layers)]
    arrives = {}
    fresh = {}
    count = [0, 0]

    def slot(q):
        count[kind_of(q)] += 1
        return kind_of(q), count[kind_of(q)] - 1

    for s in items:
        arrives[s] = slot(s[2])
    for s in items:
        if (s[0], s[1] + 1, s[2]) not in arrives:
            fresh[s] = slot(s[2])
    return items, finals, arrives, fresh, count


def grouped(number, size, alone):
    of, lengths = [], []
    for k in range(number):
        if k < number - alone and k % size:
            lengths[-1] += 1
        else:
            lengths.append(1)
        of.append(len(lengths) - 1)
    return of, lengths


def groups_of(n, layers):
    items, finals, _, _, _ = plan(n, layers)
    pieces = len(pieces_of(layers))
    ring = grouped(len(items) // 2, 3, 3)
    of, lengths = grouped(len(items) + len(finals), 12, 6)
    terms = [len(lengths) - 1 - k for k in reversed(of)], lengths[::-1]
    return ring, terms, grouped((n // 2 - 1) * pieces, 6, 3)


def waited(ref, sem):
    pltpu.make_async_copy(ref, ref, sem).wait()


def kernel(n, count_all, *refs):
    g, w, m, v, t = (refs[i : i + 3] for i in range(0, 15, 3))
    xs, ms, vs, own_new = (refs[i : i + 2] for i in range(15, 23, 2))
    far = {way: refs[23 + 2 * way : 25 + 2 * way] for way in WAYS}
    near = {way: refs[27 + 2 * way : 29 + 2 * way] for way in WAYS}
    landed, st_own, st_other, old = (refs[i : i + 2] for i in range(31, 39, 2))
    squares, rs_send, rs_recv, x_send, x_recv, st_sem, ag_send, ag_recv, y_send, y_recv, sq_send, sq_recv, in_sem = refs[39:]

    layers = m[0].shape[0]
    rows = [a.shape[1] for a in m]
    items, finals, arrives, fresh, _ = plan(n, layers)
    pieces = pieces_of(layers)
    todo = items + finals
    half = n // 2
    devices = n * CORES
    ring_groups, term_groups, gather_groups = groups_of(n, layers)
    met = set()

    def arrive(name, sem, groups, way, k):
        of, lengths = groups
        if (name, way, of[k]) not in met:
            met.add((name, way, of[k]))
            waited(landed[0].at[pl.ds(0, lengths[of[k]])], sem.at[way * len(lengths) + of[k]])

    me = lax.axis_index("dp")
    z, c = me // CORES, me % CORES
    at = lambda chip, core: lax.rem(chip + n, n) * CORES + core
    partner = at(z, 1 - c)
    ahead = {PLUS: at(z + 1, c), MINUS: at(z - 1, c)}
    step = {PLUS: 1, MINUS: -1}

    def rows_of(q, owner):
        size = rows[q[0]] // PARTS
        return pl.ds(pl.multiple_of(owner * rows[q[0]] + q[2] * size, size), size)

    def block(ref, q, owner):
        return ref[q[0]].at[q[1], rows_of(q, owner)]

    def term(q, owner):
        return g[q[0]].at[0, q[1], rows_of(q, owner)]

    def kept(pair, q):
        kind, k = place(q, pieces)
        return pair[kind].at[k]

    def remote(src, dst, send, recv, to):
        return pltpu.make_async_remote_copy(src_ref=src, dst_ref=dst, send_sem=send, recv_sem=recv, device_id={"dp": to}, device_id_type=MESH)

    x_at = []
    for _, _, q in todo:
        x_at.append((kind_of(q), sum(kind == kind_of(q) for kind, _ in x_at)))
    depth = [ref.shape[0] for ref in st_own]

    def early(i):
        return x_at[i][1] < depth[x_at[i][0]]

    def target(way, d):
        return z if way is None else z + step[way] * d

    def exchange(i):
        way, d, q = todo[i]
        kind, k = x_at[i]
        dst = (st_other if early(i) else xs)[kind].at[k]
        return remote(term(q, at(target(way, d), 1 - c)), dst, x_send.at[kind], x_recv.at[term_groups[0][i]], partner)

    def stage(i):
        way, d, q = todo[i]
        kind, k = x_at[i]
        s = k % depth[kind]
        sem = kind * depth[0] + s
        own = pltpu.make_async_copy(term(q, at(target(way, d), c)), st_own[kind].at[s], st_sem.at[0, sem])
        return [own] if early(i) else [own, pltpu.make_async_copy(xs[kind].at[k], st_other[kind].at[s], st_sem.at[1, sem])]

    def stage_start(i):
        if not early(i):
            arrive("term", x_recv, term_groups, 0, i)
        for copy in stage(i):
            copy.start()

    def slices(kind, shape, size):
        if kind:
            r = max(16, size // shape[1])
            return shape[0] // r, lambda j: (pl.ds(pl.multiple_of(j * r, r), r), slice(None))
        cols = max(128, size // shape[0])
        return shape[1] // cols, lambda j: (slice(None), pl.ds(pl.multiple_of(j * cols, cols), cols))

    def added(dst, terms, kind, total=None):
        cuts, cut = slices(kind, dst.shape, 16384)

        def one(j, acc):
            part = cut(j)
            s = terms[0][part].astype(jnp.float32)
            for r in terms[1:]:
                s = s + r[part].astype(jnp.float32)
            s = s.astype(dst.dtype)
            dst[part] = s
            if acc is None:
                return None
            s = s.astype(jnp.float32)
            s = s * s
            s = jnp.sum(s.reshape(s.shape[0] // 8, 8, s.shape[1]), axis=0)
            for k in range(s.shape[1] // 128):
                acc = acc + s[:, k * 128 : (k + 1) * 128]
            return acc

        return lax.fori_loop(0, cuts, one, total)

    def ring(s):
        way, d, q = s
        kind, k = fresh[s] if s in fresh else arrives[(way, d + 1, q)]
        to_kind, to = arrives[s]
        group = way * len(ring_groups[1]) + ring_groups[0][items.index(s) // 2]
        return remote(landed[kind].at[k], landed[to_kind].at[to], rs_send.at[kind], rs_recv.at[group], ahead[way])

    def ring_arrive(s):
        arrive("ring", rs_recv, ring_groups, s[0], items.index(s) // 2)

    def load_state(e):
        q = pieces[e]
        part = (q[1], pl.ds(q[2] * (rows[q[0]] // PARTS), rows[q[0]] // PARTS))
        return (
            pltpu.make_async_copy(m[q[0]].at[part], kept(ms, q), in_sem.at[0, kind_of(q)]),
            pltpu.make_async_copy(v[q[0]].at[part], kept(vs, q), in_sem.at[1, kind_of(q)]),
            pltpu.make_async_copy(block(w, q, me), kept(old, q), in_sem.at[2, kind_of(q)]),
        )

    window, reach = 24, 3
    first = [i for i in range(len(todo)) if early(i)]
    for i in first:
        stage_start(i)
    barrier = pltpu.get_barrier_semaphore()
    for to in (partner, ahead[PLUS], ahead[MINUS]):
        pl.semaphore_signal(barrier, inc=1, device_id={"dp": to}, device_id_type=MESH)
    pl.semaphore_wait(barrier, 3)
    for i in range(window):
        exchange(i).start()
    total = jnp.zeros((8, 128), jnp.float32)
    for i, s in enumerate(todo):
        way, d, q = s
        kind, k = x_at[i]
        if early(i):
            arrive("term", x_recv, term_groups, 0, i)
        for copy in stage(i):
            copy.wait()
        terms = [st_own[kind].at[k % depth[kind]], st_other[kind].at[k % depth[kind]]]
        if way is not None:
            if s not in fresh:
                ring_arrive((way, d + 1, q))
                kind, k = arrives[(way, d + 1, q)]
                terms.append(landed[kind].at[k])
            else:
                kind, k = fresh[s]
            added(landed[kind].at[k], terms, kind)
            ring(s).start()
        else:
            for from_ in WAYS:
                ring_arrive((from_, 1, q))
                kind, k = arrives[(from_, 1, q)]
                terms.append(landed[kind].at[k])
            total = added(kept(own_new, q), terms, kind, total)
        if i + window < len(todo):
            exchange(i + window).start()
        if i + reach < len(todo) and not early(i + reach):
            stage_start(i + reach)
        if 12 <= i < 12 + len(pieces):
            for copy in load_state(i - 12):
                copy.start()

    squares[me] = total

    def share(j):
        return remote(squares.at[me], squares.at[me], sq_send.at[0], sq_recv.at[0], lax.rem(me + j, devices))

    def several(number, ref):
        return ref.at[pl.ds(0, number)]

    for j in sorted(range(1, devices), key=lambda j: -min(j, devices - j)):
        share(j).start()
    for kind in (0, 1):
        waited(xs[kind], x_send.at[kind])
        waited(several(sum(kind_of(s[2]) == kind for s in items), landed[kind]), rs_send.at[kind])
        for which, pair in enumerate((ms, vs, old)):
            waited(pair[kind], in_sem.at[which, kind])
    waited(several(devices - 1, squares), sq_recv.at[0])
    everyone = jnp.sum(jnp.sum(squares[...], axis=0), axis=(0, 1), keepdims=True)
    factor = jnp.minimum(1.0, 0.5 * lax.rsqrt(jnp.broadcast_to(everyone, (8, 128)) / count_all + 1e-30))[0:1, 0:1]

    def stepped(q):
        wn, mr, vr, wr = kept(own_new, q), kept(ms, q), kept(vs, q), kept(old, q)
        cuts, cut = slices(kind_of(q), wn.shape, 8192)

        def one(j, _):
            part = cut(j)
            grad = wn[part].astype(jnp.float32) * factor
            mm = 0.9 * mr[part] + 0.1 * grad
            vv = 0.95 * vr[part] + 0.05 * grad * grad
            mr[part] = mm
            vr[part] = vv
            before = wr[part].astype(jnp.float32)
            wn[part] = (before - 0.02 * (mm * lax.rsqrt(vv + 1e-8) + 0.1 * before)).astype(wn.dtype)
            return None

        lax.fori_loop(0, cuts, one, None)

    gathers = [(way, h, q) for h in range(1, half) for q in pieces for way in WAYS]

    def lies(way, h, q, owner):
        if h < half - 1:
            return block(t, q, owner)
        which, among = (far, far_half(way, layers)) if q in far_half(way, layers) else (near, half_of(way, layers))
        kind, k = place(q, among)
        return which[way][kind].at[k]

    def pass_on(s):
        way, h, q = s
        owner = at(z - step[way] * (h - 1), c)
        group = way * len(gather_groups[1]) + gather_groups[0][gathers.index(s) // 2]
        src = kept(own_new, q) if h == 1 else block(t, q, owner)
        return remote(src, lies(way, h, q, owner), ag_send.at[kind_of(q)], ag_recv.at[group], ahead[way])

    def across(q, owner, src):
        return remote(src, block(t, q, owner), y_send.at[kind_of(q)], y_recv.at[kind_of(q)], partner)

    for q in pieces:
        stepped(q)
        for way in WAYS:
            pass_on((way, 1, q)).start()
        across(q, me, kept(own_new, q)).start()
    for i, s in enumerate(gathers):
        way, h, q = s
        owner = at(z - step[way] * h, c)
        arrive("gather", ag_recv, gather_groups, way, i // 2)
        if h + 1 < half:
            pass_on((way, h + 1, q)).start()
        if not late(n, way, h, q):
            across(q, owner, lies(way, h, q, owner)).start()
    waited(several(devices - 1, squares), sq_send.at[0])
    for kind in (0, 1):
        number = sum(kind_of(s[2]) == kind for s in gathers)
        waited(several(number, landed[kind]), ag_send.at[kind])
        number += sum(kind_of(q) == kind for q in pieces) - sum(kind_of(s[2]) == kind and late(n, *s) for s in gathers)
        waited(several(number, landed[kind]), y_send.at[kind])
        waited(several(number, landed[kind]), y_recv.at[kind])


READS = 4


def moved(sem, through=(), buf=None, direct=()):
    reads = -(-len(through) // READS)
    for j, (a, _) in enumerate(through):
        pltpu.make_async_copy(a, buf.at[j], sem.at[j // READS]).start()
    for k, (copies, _) in enumerate(direct):
        for a, b in copies:
            pltpu.make_async_copy(a, b, sem.at[reads + 1 + k]).start()
    for i in range(reads):
        these = range(i * READS, min(len(through), (i + 1) * READS))
        waited(buf.at[pl.ds(i * READS, len(these))], sem.at[i])
        for j in these:
            pltpu.make_async_copy(buf.at[j], through[j][1], sem.at[reads]).start()
    if through:
        waited(buf, sem.at[reads])
    for k, (_, total) in enumerate(direct):
        waited(total, sem.at[reads + 1 + k])


def row_part(ref, layer, part, rows, owner):
    size = rows // PARTS
    return ref.at[layer, pl.ds(pl.multiple_of(owner * rows + part * size, size), size)]


def moment_copies(pair, results, layers):
    pieces = pieces_of(layers)
    sets = [([], pair[0]), ([], pair[1])]
    for q in pieces:
        a, layer, part = q
        kind, k = place(q, pieces)
        size = results[a].shape[1] // PARTS
        sets[kind][0].append((pair[kind].at[k], results[a].at[layer, pl.ds(part * size, size)]))
    return sets


def settle(n, layers, arrays, rows, moments, lates, *refs):
    refs = list(refs)
    take = lambda number: [refs.pop(0) for _ in range(number)]
    t, own, far, near = take(len(arrays)), take(1)[0], take(2), take(2)
    pairs, crossed = [take(2) for _ in range(moments)], take(lates)
    outs, results = take(len(arrays)), [take(3) for _ in range(moments)]
    buf, sem = refs
    half = n // 2
    me = lax.axis_index("dp")
    z, c = me // CORES, me % CORES
    pieces = pieces_of(layers)
    through, held = [], []
    for off in range(n):
        if off == half:
            continue
        for core in range(CORES):
            owner = lax.rem(z + off, n) * CORES + (c if core == 0 else 1 - c)
            for q in pieces:
                a, layer, part = q
                if a not in arrays:
                    continue
                dst = row_part(outs[arrays.index(a)], layer, part, rows, owner)
                src = None
                if core == 0 and off == 0:
                    src = own.at[place(q, pieces)[1]]
                for way, come in ((PLUS, n - (half - 1)), (MINUS, half - 1)):
                    if off == come:
                        which, among = (far, far_half(way, layers)) if q in far_half(way, layers) else (near, half_of(way, layers))
                        if core == 0:
                            src = which[way].at[place(q, among)[1]]
                        elif late(n, way, half - 1, q):
                            src = crossed[way].at[place(q, among)[1]]
                if src is not None:
                    held.append((src, dst))
                else:
                    through.append((row_part(t[arrays.index(a)], layer, part, rows, owner), dst))
    direct = [(held, buf.at[pl.ds(0, len(held))])]
    for pair, one in zip(pairs, results, strict=True):
        direct += moment_copies(pair, one, layers)
    moved(sem, through, buf, direct)


def complete(n, layers, arrays, rows, *refs):
    k = len(arrays)
    came, outs, sem = refs[k : k + 4], refs[k + 4 : 2 * k + 4], refs[2 * k + 4]
    me = lax.axis_index("dp")
    z, c = me // CORES, me % CORES
    copies = []
    for core in range(CORES):
        owner = lax.rem(z + n // 2, n) * CORES + (c if core == 0 else 1 - c)
        for way in WAYS:
            for q in far_half(way, layers):
                if q[0] in arrays:
                    src = came[2 * core + way].at[place(q, far_half(way, layers))[1]]
                    copies.append((src, row_part(outs[arrays.index(q[0])], q[1], q[2], rows, owner)))
    moved(sem, direct=[(copies, outs[0].at[0, pl.ds(0, len(copies) * (rows // PARTS))])])


def solution(mesh):
    devices = mesh.shape["dp"]
    n = devices // CORES
    hbm, vmem = pl.BlockSpec(memory_space=pltpu.HBM), pl.BlockSpec(memory_space=pltpu.VMEM)
    bf, f32 = jnp.bfloat16, jnp.float32
    dma = pltpu.SemaphoreType.DMA
    like = lambda a: jax.ShapeDtypeStruct(a.shape, a.dtype)

    def params(mib, **more):
        return pltpu.CompilerParams(vmem_limit_bytes=mib * 2**20, **more)

    def summed(terms, weights, m, v):
        layers = m[0].shape[0]
        items, finals, _, _, count = plan(n, layers)
        pieces = pieces_of(layers)
        todo = items + finals
        shapes = [(m[a].shape[1] // PARTS, m[a].shape[2]) for a in (0, DOWN)]
        pair = lambda make, number, dtype: [make((number[kind], *shapes[kind]), dtype) for kind in (0, 1)]
        whole, part = counts(pieces), counts(half_of(PLUS, layers))
        ring_groups, term_groups, gather_groups = groups_of(n, layers)
        outs = [like(w) for w in weights] + pair(jax.ShapeDtypeStruct, counts([s[2] for s in todo]), bf)
        held = 2 * pair(pltpu.VMEM, whole, f32) + pair(pltpu.VMEM, whole, bf) + 4 * pair(pltpu.VMEM, part, bf)
        return pl.pallas_call(
            functools.partial(kernel, n, devices * sum(one.size for one in m)),
            out_shape=outs + held,
            in_specs=[hbm] * 12,
            out_specs=[hbm] * len(outs) + [vmem] * len(held),
            scratch_shapes=pair(pltpu.VMEM, count, bf)
            + 2 * pair(pltpu.VMEM, (4, 2), bf)
            + pair(pltpu.VMEM, whole, bf)
            + [pltpu.VMEM((devices, 8, 128), f32)]
            + [dma((2,)), dma((2 * len(ring_groups[1]),))]
            + [dma((2,)), dma((len(term_groups[1]),))]
            + [dma((2, 6))]
            + [dma((2,)), dma((2 * len(gather_groups[1]),))]
            + [dma((2,)), dma((2,))]
            + [dma((1,)), dma((1,))]
            + [dma((3, 2))],
            compiler_params=params(34, collective_id=0, has_side_effects=True),
            name="summed",
        )(*terms, *weights, *m, *v)

    def settled(arrays, t, own, far, near, m, moments=(), crossed=()):
        layers, rows = m[0].shape[0], m[arrays[0]].shape[1]
        jobs = (n - 1) * CORES * len(arrays) * layers * PARTS
        held = 3 * len(arrays) * layers * PARTS + sum(one.shape[0] for one in crossed)
        through = jobs - held
        size = rows // PARTS * t[0].shape[2]
        moved_bytes = 2 * size * (jobs + through) + sum(4 * one.size for pair in moments for one in pair)
        results = [like(one) for _ in moments for one in m]
        return pl.pallas_call(
            functools.partial(settle, n, layers, arrays, rows, len(moments), len(crossed)),
            out_shape=[like(one) for one in t] + results,
            in_specs=[hbm] * len(t) + [vmem] * (5 + 2 * len(moments) + len(crossed)),
            out_specs=[hbm] * (len(t) + len(results)),
            scratch_shapes=[pltpu.VMEM((through, rows // PARTS, t[0].shape[2]), bf), dma((-(-through // READS) + 2 + 2 * len(moments),))],
            compiler_params=params(2 * size * through // 2**20 + 2),
            cost_estimate=pl.CostEstimate(flops=60 * moved_bytes, bytes_accessed=moved_bytes, transcendentals=0),
            name="settle",
        )(*(pltpu.with_memory_space_constraint(one, pltpu.HBM) for one in t), own, *far, *near, *(one for pair in moments for one in pair), *crossed)

    def completed(arrays, results, came, rows):
        layers = results[0].shape[0]
        return pl.pallas_call(
            functools.partial(complete, n, layers, arrays, rows),
            out_shape=[like(one) for one in results],
            in_specs=[hbm] * len(results) + [vmem] * 4,
            out_specs=[hbm] * len(results),
            scratch_shapes=[dma((2,))],
            input_output_aliases={i: i for i in range(len(results))},
            compiler_params=params(16),
            name="complete",
        )(*results, *came)

    def step(*arrays):
        terms, weights, m, v = (arrays[i : i + 3] for i in (0, 3, 6, 9))
        out = summed(terms, weights, m, v)
        t = out[:3]
        new_m, new_v, own = (out[i : i + 2] for i in (5, 7, 9))
        far, near = (out[11], out[13], out[12], out[14]), (out[15], out[17], out[16], out[18])
        onward = [(i, (i + CORES) % devices) for i in range(devices)]
        back = [(b, a) for a, b in onward]
        other = [(i, i + 1 - 2 * (i % CORES)) for i in range(devices)]

        def hop(k):
            return [lax.ppermute(one, "dp", way) for one, way in zip(far[k : k + 2], (onward, back), strict=True)]

        def cross(came):
            return came + [lax.ppermute(one, "dp", other) for one in came]

        rows = [one.shape[1] for one in m]
        wide = hop(0)
        down = hop(2)
        crossed = [lax.ppermute(one, "dp", other) for one in (far[2 + PLUS], near[2 + MINUS])]
        new_g, new_u, *moments = settled((0, 1), t[:2], own[0], far[:2], near[:2], m, (new_m, new_v))
        (new_d,) = settled((2,), t[2:], own[1], far[2:], near[2:], m, (), crossed)
        wide = cross(wide)
        down = cross(down)
        new_g, new_u = completed((0, 1), (new_g, new_u), wide, rows[0])
        (new_d,) = completed((2,), (new_d,), down, rows[2])
        return (new_g, new_u, new_d, *moments)

    all_of, cut = P(None, None, None), P(None, "dp", None)
    return jax.shard_map(
        step,
        mesh=mesh,
        in_specs=(P(("rep", "dp"), None, None, None),) * 3 + (all_of,) * 3 + (cut,) * 6,
        out_specs=(P("rep", None, None),) * 3 + (P("rep", "dp", None),) * 6,
        check_vma=False,
    )
```

```python
import functools

import jax
import jax.numpy as jnp
from jax import lax
from jax.experimental import pallas as pl
from jax.experimental.pallas import tpu as pltpu
from jax.sharding import PartitionSpec as P


MESH = pl.DeviceIdType.MESH
CORES = 2
PLUS, MINUS = WAYS = 0, 1
PARTS = 2
LEAD = 2
DOWN = 2


def pieces_of(layers):
    return [(a, layer, part) for part in range(PARTS) for layer in range(layers) for a in range(3)]


def kind_of(q):
    return int(q[0] == DOWN)


def place(q, among):
    return kind_of(q), [p for p in among if kind_of(p) == kind_of(q)].index(q)


def counts(among):
    return [sum(kind_of(q) == kind for q in among) for kind in (0, 1)]


def half_of(way, layers):
    return [q for q in pieces_of(layers) if q[2] % 2 == way]


def far_half(way, layers):
    return half_of(1 - way, layers)


def late(n, way, h, q):
    return h == n // 2 - 1 and q[0] == DOWN and q[2] == PARTS - 1


def plan(n, layers):
    half = n // 2
    queue = {}
    for way in WAYS:
        mine, other = half_of(way, layers), half_of(1 - way, layers)
        sends = [(way, half, q) for q in mine]
        for d in range(half - 1, 0, -1):
            sends += [(way, d, q) for q in (other + mine if d > 1 else pieces_of(layers))]
        queue[way] = sends
    items = [s for pair in zip(queue[PLUS], queue[MINUS], strict=True) for s in pair]
    finals = [(None, 0, q) for q in pieces_of(layers)]
    arrives = {}
    fresh = {}
    count = [0, 0]

    def slot(q):
        count[kind_of(q)] += 1
        return kind_of(q), count[kind_of(q)] - 1

    for s in items:
        arrives[s] = slot(s[2])
    for s in items:
        if (s[0], s[1] + 1, s[2]) not in arrives:
            fresh[s] = slot(s[2])
    return items, finals, arrives, fresh, count


def grouped(number, size, alone):
    of, lengths = [], []
    for k in range(number):
        if k < number - alone and k % size:
            lengths[-1] += 1
        else:
            lengths.append(1)
        of.append(len(lengths) - 1)
    return of, lengths


def groups_of(n, layers):
    items, finals, _, _, _ = plan(n, layers)
    pieces = len(pieces_of(layers))
    ring = grouped(len(items) // 2, 3, 3)
    of, lengths = grouped(len(items) + len(finals), 12, 6)
    terms = [len(lengths) - 1 - k for k in reversed(of)], lengths[::-1]
    return ring, terms, grouped((n // 2 - 1) * pieces, 6, 3)


def waited(ref, sem):
    pltpu.make_async_copy(ref, ref, sem).wait()


def kernel(n, count_all, *refs):
    g, w, m, v, t = (refs[i : i + 3] for i in range(0, 15, 3))
    xs, ms, vs, own_new = (refs[i : i + 2] for i in range(15, 23, 2))
    far = {way: refs[23 + 2 * way : 25 + 2 * way] for way in WAYS}
    near = {way: refs[27 + 2 * way : 29 + 2 * way] for way in WAYS}
    landed, st_own, st_other = (refs[i : i + 2] for i in range(31, 37, 2))
    squares, lead, rs_send, rs_recv, x_send, x_recv, st_sem, ag_send, ag_recv, y_send, y_recv, sq_send, sq_recv, in_sem, lead_sem = refs[37:]

    layers = m[0].shape[0]
    rows = [a.shape[1] for a in m]
    items, finals, arrives, fresh, _ = plan(n, layers)
    pieces = pieces_of(layers)
    todo = items + finals
    half = n // 2
    devices = n * CORES
    ring_groups, term_groups, gather_groups = groups_of(n, layers)
    met = set()

    def arrive(name, sem, groups, way, k):
        of, lengths = groups
        if (name, way, of[k]) not in met:
            met.add((name, way, of[k]))
            waited(landed[0].at[pl.ds(0, lengths[of[k]])], sem.at[way * len(lengths) + of[k]])

    me = lax.axis_index("dp")
    z, c = me // CORES, me % CORES
    at = lambda chip, core: lax.rem(chip + n, n) * CORES + core
    partner = at(z, 1 - c)
    ahead = {PLUS: at(z + 1, c), MINUS: at(z - 1, c)}
    step = {PLUS: 1, MINUS: -1}

    def rows_of(q, owner):
        size = rows[q[0]] // PARTS
        return pl.ds(pl.multiple_of(owner * rows[q[0]] + q[2] * size, size), size)

    def block(ref, q, owner):
        return ref[q[0]].at[q[1], rows_of(q, owner)]

    def term(q, owner):
        return g[q[0]].at[0, q[1], rows_of(q, owner)]

    def kept(pair, q):
        kind, k = place(q, pieces)
        return pair[kind].at[k]

    def remote(src, dst, send, recv, to):
        return pltpu.make_async_remote_copy(src_ref=src, dst_ref=dst, send_sem=send, recv_sem=recv, device_id={"dp": to}, device_id_type=MESH)

    x_at = []
    for _, _, q in todo:
        x_at.append((kind_of(q), sum(kind == kind_of(q) for kind, _ in x_at)))
    depth = [ref.shape[0] for ref in st_own]

    def early(i):
        return x_at[i][1] < depth[x_at[i][0]]

    def target(way, d):
        return z if way is None else z + step[way] * d

    def exchange(i):
        way, d, q = todo[i]
        kind, k = x_at[i]
        dst = (st_other if early(i) else xs)[kind].at[k]
        src = lead.at[i] if i < LEAD else term(q, at(target(way, d), 1 - c))
        return remote(src, dst, x_send.at[kind], x_recv.at[term_groups[0][i]], partner)

    def lead_in(i):
        way, d, q = todo[i]
        return pltpu.make_async_copy(term(q, at(target(way, d), 1 - c)), lead.at[i], lead_sem.at[i])

    def stage(i):
        way, d, q = todo[i]
        kind, k = x_at[i]
        s = k % depth[kind]
        sem = kind * depth[0] + s
        own = pltpu.make_async_copy(term(q, at(target(way, d), c)), st_own[kind].at[s], st_sem.at[0, sem])
        return [own] if early(i) else [own, pltpu.make_async_copy(xs[kind].at[k], st_other[kind].at[s], st_sem.at[1, sem])]

    def stage_start(i):
        if not early(i):
            arrive("term", x_recv, term_groups, 0, i)
        for copy in stage(i):
            copy.start()

    def slices(kind, shape, size):
        if kind:
            r = max(16, size // shape[1])
            return shape[0] // r, lambda j: (pl.ds(pl.multiple_of(j * r, r), r), slice(None))
        cols = max(128, size // shape[0])
        return shape[1] // cols, lambda j: (slice(None), pl.ds(pl.multiple_of(j * cols, cols), cols))

    def added(dst, terms, kind, total=None):
        cuts, cut = slices(kind, dst.shape, 16384)

        def one(j, acc):
            part = cut(j)
            s = terms[0][part].astype(jnp.float32)
            for r in terms[1:]:
                s = s + r[part].astype(jnp.float32)
            s = s.astype(dst.dtype)
            dst[part] = s
            if acc is None:
                return None
            s = s.astype(jnp.float32)
            s = s * s
            s = jnp.sum(s.reshape(s.shape[0] // 8, 8, s.shape[1]), axis=0)
            for k in range(s.shape[1] // 128):
                acc = acc + s[:, k * 128 : (k + 1) * 128]
            return acc

        return lax.fori_loop(0, cuts, one, total)

    def ring(s):
        way, d, q = s
        kind, k = fresh[s] if s in fresh else arrives[(way, d + 1, q)]
        to_kind, to = arrives[s]
        group = way * len(ring_groups[1]) + ring_groups[0][items.index(s) // 2]
        return remote(landed[kind].at[k], landed[to_kind].at[to], rs_send.at[kind], rs_recv.at[group], ahead[way])

    def ring_arrive(s):
        arrive("ring", rs_recv, ring_groups, s[0], items.index(s) // 2)

    def load_state(e):
        q = pieces[e]
        part = (q[1], pl.ds(q[2] * (rows[q[0]] // PARTS), rows[q[0]] // PARTS))
        return (
            pltpu.make_async_copy(m[q[0]].at[part], kept(ms, q), in_sem.at[0, kind_of(q)]),
            pltpu.make_async_copy(v[q[0]].at[part], kept(vs, q), in_sem.at[1, kind_of(q)]),
        )

    def old(q):
        kind, k = place(q, pieces)
        return st_own[kind].at[k] if k < depth[kind] else st_other[kind].at[k - depth[kind]]

    def load_weight(q):
        return pltpu.make_async_copy(block(w, q, me), old(q), in_sem.at[2, kind_of(q)])

    window, reach = 24, 3
    for i in range(LEAD):
        lead_in(i).start()
    first = [i for i in range(len(todo)) if early(i)]
    for i in first:
        stage_start(i)
    barrier = pltpu.get_barrier_semaphore()
    for to in (partner, ahead[PLUS], ahead[MINUS]):
        pl.semaphore_signal(barrier, inc=1, device_id={"dp": to}, device_id_type=MESH)
    pl.semaphore_wait(barrier, 3)
    for i in range(window):
        if i < LEAD:
            lead_in(i).wait()
        exchange(i).start()
    total = jnp.zeros((8, 128), jnp.float32)
    for i, s in enumerate(todo):
        way, d, q = s
        kind, k = x_at[i]
        if early(i):
            arrive("term", x_recv, term_groups, 0, i)
        for copy in stage(i):
            copy.wait()
        terms = [st_own[kind].at[k % depth[kind]], st_other[kind].at[k % depth[kind]]]
        if way is not None:
            if s not in fresh:
                ring_arrive((way, d + 1, q))
                kind, k = arrives[(way, d + 1, q)]
                terms.append(landed[kind].at[k])
            else:
                kind, k = fresh[s]
            added(landed[kind].at[k], terms, kind)
            ring(s).start()
        else:
            for from_ in WAYS:
                ring_arrive((from_, 1, q))
                kind, k = arrives[(from_, 1, q)]
                terms.append(landed[kind].at[k])
            total = added(kept(own_new, q), terms, kind, total)
        if i + window < len(todo):
            exchange(i + window).start()
        if i + reach < len(todo) and not early(i + reach):
            stage_start(i + reach)
        if 12 <= i < 12 + len(pieces):
            for copy in load_state(i - 12):
                copy.start()

    squares[me] = total

    def share(j):
        return remote(squares.at[me], squares.at[me], sq_send.at[0], sq_recv.at[0], lax.rem(me + j, devices))

    def several(number, ref):
        return ref.at[pl.ds(0, number)]

    for j in sorted(range(1, devices), key=lambda j: -min(j, devices - j)):
        share(j).start()
    for q in pieces:
        load_weight(q).start()
    for kind in (0, 1):
        waited(xs[kind], x_send.at[kind])
        waited(several(sum(kind_of(s[2]) == kind for s in items), landed[kind]), rs_send.at[kind])
        for which, pair in enumerate((ms, vs, own_new)):
            waited(pair[kind], in_sem.at[which, kind])
    waited(several(devices - 1, squares), sq_recv.at[0])
    everyone = jnp.sum(jnp.sum(squares[...], axis=0), axis=(0, 1), keepdims=True)
    factor = jnp.minimum(1.0, 0.5 * lax.rsqrt(jnp.broadcast_to(everyone, (8, 128)) / count_all + 1e-30))[0:1, 0:1]

    def stepped(q, share_of=(0, 1)):
        wn, mr, vr, wr = kept(own_new, q), kept(ms, q), kept(vs, q), old(q)
        cuts, cut = slices(kind_of(q), wn.shape, 8192)

        def one(j, _):
            part = cut(j)
            grad = wn[part].astype(jnp.float32) * factor
            mm = 0.9 * mr[part] + 0.1 * grad
            vv = 0.95 * vr[part] + 0.05 * grad * grad
            mr[part] = mm
            vr[part] = vv
            before = wr[part].astype(jnp.float32)
            wn[part] = (before - 0.02 * (mm * lax.rsqrt(vv + 1e-8) + 0.1 * before)).astype(wn.dtype)
            return None

        lax.fori_loop(cuts * share_of[0] // share_of[1], cuts * (share_of[0] + 1) // share_of[1], one, None)

    gathers = [(way, h, q) for h in range(1, half) for q in pieces for way in WAYS]

    def lies(way, h, q, owner):
        if h < half - 1:
            return block(t, q, owner)
        which, among = (far, far_half(way, layers)) if q in far_half(way, layers) else (near, half_of(way, layers))
        kind, k = place(q, among)
        return which[way][kind].at[k]

    def pass_on(s, columns=None):
        way, h, q = s
        owner = at(z - step[way] * (h - 1), c)
        group = way * len(gather_groups[1]) + gather_groups[0][gathers.index(s) // 2]
        src = kept(own_new, q) if h == 1 else lies(way, h - 1, q, owner)
        dst = lies(way, h, q, owner)
        if columns is not None:
            src, dst = src.at[:, columns], dst.at[:, columns]
        return remote(src, dst, ag_send.at[kind_of(q)], ag_recv.at[group], ahead[way])

    def across(q, owner, src):
        return remote(src, block(t, q, owner), y_send.at[kind_of(q)], y_recv.at[kind_of(q)], partner)

    for q in pieces:
        quarter = t[0].shape[2] // 4
        for k in range(4 if q == pieces[0] else 0):
            stepped(q, (k, 4))
            for way in WAYS:
                pass_on((way, 1, q), pl.ds(k * quarter, quarter)).start()
        if q != pieces[0]:
            stepped(q)
            for way in WAYS:
                pass_on((way, 1, q)).start()
        across(q, me, kept(own_new, q)).start()
    for i, s in enumerate(gathers):
        way, h, q = s
        owner = at(z - step[way] * h, c)
        arrive("gather", ag_recv, gather_groups, way, i // 2)
        if h + 1 < half:
            pass_on((way, h + 1, q)).start()
        if not late(n, way, h, q):
            across(q, owner, lies(way, h, q, owner)).start()
    waited(several(devices - 1, squares), sq_send.at[0])
    for kind in (0, 1):
        number = sum(kind_of(s[2]) == kind for s in gathers)
        waited(several(number, landed[kind]), ag_send.at[kind])
        number += sum(kind_of(q) == kind for q in pieces) - sum(kind_of(s[2]) == kind and late(n, *s) for s in gathers)
        waited(several(number, landed[kind]), y_send.at[kind])
        waited(several(number, landed[kind]), y_recv.at[kind])


READS = 4


def moved(sem, through=(), buf=None, direct=()):
    reads = -(-len(through) // READS)
    for j, (a, _) in enumerate(through):
        pltpu.make_async_copy(a, buf.at[j], sem.at[j // READS]).start()
    for k, (copies, _) in enumerate(direct):
        for a, b in copies:
            pltpu.make_async_copy(a, b, sem.at[reads + 1 + k]).start()
    for i in range(reads):
        these = range(i * READS, min(len(through), (i + 1) * READS))
        waited(buf.at[pl.ds(i * READS, len(these))], sem.at[i])
        for j in these:
            pltpu.make_async_copy(buf.at[j], through[j][1], sem.at[reads]).start()
    if through:
        waited(buf, sem.at[reads])
    for k, (_, total) in enumerate(direct):
        waited(total, sem.at[reads + 1 + k])


def row_part(ref, layer, part, rows, owner):
    size = rows // PARTS
    return ref.at[layer, pl.ds(pl.multiple_of(owner * rows + part * size, size), size)]


def moment_copies(pair, results, layers):
    pieces = pieces_of(layers)
    sets = [([], pair[0]), ([], pair[1])]
    for q in pieces:
        a, layer, part = q
        kind, k = place(q, pieces)
        size = results[a].shape[1] // PARTS
        sets[kind][0].append((pair[kind].at[k], results[a].at[layer, pl.ds(part * size, size)]))
    return sets


def settle(n, layers, arrays, rows, moments, *refs):
    refs = list(refs)
    take = lambda number: [refs.pop(0) for _ in range(number)]
    t, own, far, near = take(len(arrays)), take(1)[0], take(2), take(2)
    pairs = [take(2) for _ in range(moments)]
    outs, results = take(len(arrays)), [take(3) for _ in range(moments)]
    buf, sem = refs
    half = n // 2
    me = lax.axis_index("dp")
    z, c = me // CORES, me % CORES
    pieces = pieces_of(layers)
    through, held = [], []
    for off in range(n):
        if off == half:
            continue
        for core in range(CORES):
            owner = lax.rem(z + off, n) * CORES + (c if core == 0 else 1 - c)
            for q in pieces:
                a, layer, part = q
                if a not in arrays:
                    continue
                dst = row_part(outs[arrays.index(a)], layer, part, rows, owner)
                src, left = None, False
                if core == 0 and off == 0:
                    src = own.at[place(q, pieces)[1]]
                for way in WAYS:
                    hops = n - off if way == PLUS else off
                    if hops == half - 1 and core == 0:
                        which, among = (far, far_half(way, layers)) if q in far_half(way, layers) else (near, half_of(way, layers))
                        src = which[way].at[place(q, among)[1]]
                    left = left or (core == 1 and late(n, way, hops, q))
                if left:
                    continue
                if src is not None:
                    held.append((src, dst))
                else:
                    through.append((row_part(t[arrays.index(a)], layer, part, rows, owner), dst))
    direct = [(held, buf.at[pl.ds(0, len(held))])]
    for pair, one in zip(pairs, results, strict=True):
        direct += moment_copies(pair, one, layers)
    moved(sem, through, buf, direct)


def complete(n, layers, arrays, rows, lates, *refs):
    k = len(arrays)
    came, crossed = refs[k : k + 4], refs[k + 4 : k + 4 + lates]
    outs, sem = refs[k + 4 + lates : 2 * k + 4 + lates], refs[2 * k + 4 + lates]
    me = lax.axis_index("dp")
    z, c = me // CORES, me % CORES
    copies = []
    for core in range(CORES):
        owner = lax.rem(z + n // 2, n) * CORES + (c if core == 0 else 1 - c)
        for way in WAYS:
            for q in far_half(way, layers):
                if q[0] in arrays:
                    src = came[2 * core + way].at[place(q, far_half(way, layers))[1]]
                    copies.append((src, row_part(outs[arrays.index(q[0])], q[1], q[2], rows, owner)))
    hops = n // 2 - 1
    for way, ref in zip(WAYS, crossed):
        owner = lax.rem(z + (n - hops if way == PLUS else hops), n) * CORES + 1 - c
        for q in pieces_of(layers):
            if late(n, way, hops, q):
                among = far_half(way, layers) if q in far_half(way, layers) else half_of(way, layers)
                copies.append((ref.at[place(q, among)[1]], row_part(outs[arrays.index(q[0])], q[1], q[2], rows, owner)))
    moved(sem, direct=[(copies, outs[0].at[0, pl.ds(0, len(copies) * (rows // PARTS))])])


def solution(mesh):
    devices = mesh.shape["dp"]
    n = devices // CORES
    hbm, vmem = pl.BlockSpec(memory_space=pltpu.HBM), pl.BlockSpec(memory_space=pltpu.VMEM)
    bf, f32 = jnp.bfloat16, jnp.float32
    dma = pltpu.SemaphoreType.DMA
    like = lambda a: jax.ShapeDtypeStruct(a.shape, a.dtype)

    def params(mib, **more):
        return pltpu.CompilerParams(vmem_limit_bytes=mib * 2**20, **more)

    def summed(terms, weights, m, v):
        layers = m[0].shape[0]
        items, finals, _, _, count = plan(n, layers)
        pieces = pieces_of(layers)
        todo = items + finals
        shapes = [(m[a].shape[1] // PARTS, m[a].shape[2]) for a in (0, DOWN)]
        pair = lambda make, number, dtype: [make((number[kind], *shapes[kind]), dtype) for kind in (0, 1)]
        whole, part = counts(pieces), counts(half_of(PLUS, layers))
        ring_groups, term_groups, gather_groups = groups_of(n, layers)
        outs = [like(w) for w in weights] + pair(jax.ShapeDtypeStruct, counts([s[2] for s in todo]), bf)
        held = 2 * pair(pltpu.VMEM, whole, f32) + pair(pltpu.VMEM, whole, bf) + 4 * pair(pltpu.VMEM, part, bf)
        return pl.pallas_call(
            functools.partial(kernel, n, devices * sum(one.size for one in m)),
            out_shape=outs + held,
            in_specs=[hbm] * 12,
            out_specs=[hbm] * len(outs) + [vmem] * len(held),
            scratch_shapes=pair(pltpu.VMEM, count, bf)
            + 2 * pair(pltpu.VMEM, [-(-number // 2) for number in whole], bf)
            + [pltpu.VMEM((devices, 8, 128), f32), pltpu.VMEM((LEAD, *shapes[0]), bf)]
            + [dma((2,)), dma((2 * len(ring_groups[1]),))]
            + [dma((2,)), dma((len(term_groups[1]),))]
            + [dma((2, sum(-(-number // 2) for number in whole)))]
            + [dma((2,)), dma((2 * len(gather_groups[1]),))]
            + [dma((2,)), dma((2,))]
            + [dma((1,)), dma((1,))]
            + [dma((3, 2)), dma((LEAD,))],
            compiler_params=params(31, collective_id=0, has_side_effects=True),
            name="summed",
        )(*terms, *weights, *m, *v)

    def settled(arrays, t, own, far, near, m, moments=()):
        layers, rows = m[0].shape[0], m[arrays[0]].shape[1]
        jobs = (n - 1) * CORES * len(arrays) * layers * PARTS
        jobs -= sum(late(n, way, n // 2 - 1, q) and q[0] in arrays for way in WAYS for q in pieces_of(layers))
        held = 3 * len(arrays) * layers * PARTS
        through = jobs - held
        size = rows // PARTS * t[0].shape[2]
        moved_bytes = 2 * size * (jobs + through) + sum(4 * one.size for pair in moments for one in pair)
        results = [like(one) for _ in moments for one in m]
        return pl.pallas_call(
            functools.partial(settle, n, layers, arrays, rows, len(moments)),
            out_shape=[like(one) for one in t] + results,
            in_specs=[hbm] * len(t) + [vmem] * (5 + 2 * len(moments)),
            out_specs=[hbm] * (len(t) + len(results)),
            scratch_shapes=[pltpu.VMEM((through, rows // PARTS, t[0].shape[2]), bf), dma((-(-through // READS) + 2 + 2 * len(moments),))],
            compiler_params=params(-(-2 * size * through // 2**20) + 1),
            cost_estimate=pl.CostEstimate(flops=60 * moved_bytes, bytes_accessed=moved_bytes, transcendentals=0),
            name="settle",
        )(*(pltpu.with_memory_space_constraint(one, pltpu.HBM) for one in t), own, *far, *near, *(one for pair in moments for one in pair))

    def completed(arrays, results, came, rows, crossed=()):
        layers = results[0].shape[0]
        return pl.pallas_call(
            functools.partial(complete, n, layers, arrays, rows, len(crossed)),
            out_shape=[like(one) for one in results],
            in_specs=[hbm] * len(results) + [vmem] * (4 + len(crossed)),
            out_specs=[hbm] * len(results),
            scratch_shapes=[dma((2,))],
            input_output_aliases={i: i for i in range(len(results))},
            compiler_params=params(8),
            name="complete",
        )(*results, *came, *crossed)

    def step(*arrays):
        terms, weights, m, v = (arrays[i : i + 3] for i in (0, 3, 6, 9))
        out = summed(terms, weights, m, v)
        t = out[:3]
        new_m, new_v, own = (out[i : i + 2] for i in (5, 7, 9))
        far, near = (out[11], out[13], out[12], out[14]), (out[15], out[17], out[16], out[18])
        onward = [(i, (i + CORES) % devices) for i in range(devices)]
        back = [(b, a) for a, b in onward]
        other = [(i, i + 1 - 2 * (i % CORES)) for i in range(devices)]

        def hop(k):
            return [lax.ppermute(one, "dp", way) for one, way in zip(far[k : k + 2], (onward, back), strict=True)]

        def cross(came):
            return came + [lax.ppermute(one, "dp", other) for one in came]

        rows = [one.shape[1] for one in m]
        wide = hop(0)
        down = hop(2)
        crossed = [lax.ppermute(one, "dp", other) for one in (far[2 + PLUS], near[2 + MINUS])]
        new_g, new_u, *moments = settled((0, 1), t[:2], own[0], far[:2], near[:2], m, (new_m, new_v))
        (new_d,) = settled((2,), t[2:], own[1], far[2:], near[2:], m)
        wide = cross(wide)
        down = cross(down)
        new_g, new_u = completed((0, 1), (new_g, new_u), wide, rows[0])
        (new_d,) = completed((2,), (new_d,), down, rows[2], crossed)
        return (new_g, new_u, new_d, *moments)

    all_of, cut = P(None, None, None), P(None, "dp", None)
    return jax.shard_map(
        step,
        mesh=mesh,
        in_specs=(P(("rep", "dp"), None, None, None),) * 3 + (all_of,) * 3 + (cut,) * 6,
        out_specs=(P("rep", None, None),) * 3 + (P("rep", "dp", None),) * 6,
        check_vma=False,
    )
```

```python
import functools

import jax
import jax.numpy as jnp
from jax import lax
from jax.experimental import pallas as pl
from jax.experimental.pallas import tpu as pltpu
from jax.sharding import PartitionSpec as P


MESH = pl.DeviceIdType.MESH
CORES = 2
PLUS, MINUS = WAYS = 0, 1
PARTS = 2
LEAD = 2
DOWN = 2


def pieces_of(layers):
    return [(a, layer, part) for part in range(PARTS) for layer in range(layers) for a in range(3)]


def kind_of(q):
    return int(q[0] == DOWN)


def place(q, among):
    return kind_of(q), [p for p in among if kind_of(p) == kind_of(q)].index(q)


def counts(among):
    return [sum(kind_of(q) == kind for q in among) for kind in (0, 1)]


def half_of(way, layers):
    return [q for q in pieces_of(layers) if q[2] % 2 == way]


def far_half(way, layers):
    return half_of(1 - way, layers)


def late(n, way, h, q):
    return h == n // 2 - 1 and q[0] == DOWN and q[2] == PARTS - 1


def plan(n, layers):
    half = n // 2
    queue = {}
    for way in WAYS:
        mine, other = half_of(way, layers), half_of(1 - way, layers)
        sends = [(way, half, q) for q in mine]
        for d in range(half - 1, 0, -1):
            sends += [(way, d, q) for q in (other + mine if d > 1 else pieces_of(layers))]
        queue[way] = sends
    items = [s for pair in zip(queue[PLUS], queue[MINUS], strict=True) for s in pair]
    finals = [(None, 0, q) for q in pieces_of(layers)]
    arrives = {}
    fresh = {}
    count = [0, 0]

    def slot(q):
        count[kind_of(q)] += 1
        return kind_of(q), count[kind_of(q)] - 1

    for s in items:
        arrives[s] = slot(s[2])
    for s in items:
        if (s[0], s[1] + 1, s[2]) not in arrives:
            fresh[s] = slot(s[2])
    return items, finals, arrives, fresh, count


def grouped(number, size, alone):
    of, lengths = [], []
    for k in range(number):
        if k < number - alone and k % size:
            lengths[-1] += 1
        else:
            lengths.append(1)
        of.append(len(lengths) - 1)
    return of, lengths


def groups_of(n, layers):
    items, finals, _, _, _ = plan(n, layers)
    pieces = len(pieces_of(layers))
    ring = grouped(len(items) // 2, 3, 3)
    of, lengths = grouped(len(items) + len(finals), 12, 6)
    terms = [len(lengths) - 1 - k for k in reversed(of)], lengths[::-1]
    return ring, terms, grouped((n // 2 - 1) * pieces, 6, 3)


def waited(ref, sem):
    pltpu.make_async_copy(ref, ref, sem).wait()


def kernel(n, count_all, *refs):
    g, w, m, v, t = (refs[i : i + 3] for i in range(0, 15, 3))
    xs, ms, vs, own_new = (refs[i : i + 2] for i in range(15, 23, 2))
    far = {way: refs[23 + 2 * way : 25 + 2 * way] for way in WAYS}
    near = {way: refs[27 + 2 * way : 29 + 2 * way] for way in WAYS}
    middle = refs[31:33]
    landed, st_own, st_other = (refs[i : i + 2] for i in range(33, 39, 2))
    squares, lead, rs_send, rs_recv, x_send, x_recv, st_sem, ag_send, ag_recv, y_send, y_recv, sq_send, sq_recv, in_sem, lead_sem = refs[39:]

    layers = m[0].shape[0]
    rows = [a.shape[1] for a in m]
    items, finals, arrives, fresh, _ = plan(n, layers)
    pieces = pieces_of(layers)
    todo = items + finals
    half = n // 2
    devices = n * CORES
    ring_groups, term_groups, gather_groups = groups_of(n, layers)
    met = set()

    def arrive(name, sem, groups, way, k):
        of, lengths = groups
        if (name, way, of[k]) not in met:
            met.add((name, way, of[k]))
            waited(landed[0].at[pl.ds(0, lengths[of[k]])], sem.at[way * len(lengths) + of[k]])

    me = lax.axis_index("dp")
    z, c = me // CORES, me % CORES
    at = lambda chip, core: lax.rem(chip + n, n) * CORES + core
    partner = at(z, 1 - c)
    ahead = {PLUS: at(z + 1, c), MINUS: at(z - 1, c)}
    step = {PLUS: 1, MINUS: -1}

    def rows_of(q, owner):
        size = rows[q[0]] // PARTS
        return pl.ds(pl.multiple_of(owner * rows[q[0]] + q[2] * size, size), size)

    def block(ref, q, owner):
        return ref[q[0]].at[q[1], rows_of(q, owner)]

    def term(q, owner):
        return g[q[0]].at[0, q[1], rows_of(q, owner)]

    def kept(pair, q):
        kind, k = place(q, pieces)
        return pair[kind].at[k]

    def remote(src, dst, send, recv, to):
        return pltpu.make_async_remote_copy(src_ref=src, dst_ref=dst, send_sem=send, recv_sem=recv, device_id={"dp": to}, device_id_type=MESH)

    x_at = []
    for _, _, q in todo:
        x_at.append((kind_of(q), sum(kind == kind_of(q) for kind, _ in x_at)))
    depth = [ref.shape[0] for ref in st_own]

    def early(i):
        return x_at[i][1] < depth[x_at[i][0]]

    def target(way, d):
        return z if way is None else z + step[way] * d

    def exchange(i):
        way, d, q = todo[i]
        kind, k = x_at[i]
        dst = (st_other if early(i) else xs)[kind].at[k]
        src = lead.at[i] if i < LEAD else term(q, at(target(way, d), 1 - c))
        return remote(src, dst, x_send.at[kind], x_recv.at[term_groups[0][i]], partner)

    def lead_in(i):
        way, d, q = todo[i]
        return pltpu.make_async_copy(term(q, at(target(way, d), 1 - c)), lead.at[i], lead_sem.at[i])

    def stage(i):
        way, d, q = todo[i]
        kind, k = x_at[i]
        s = k % depth[kind]
        sem = kind * depth[0] + s
        own = pltpu.make_async_copy(term(q, at(target(way, d), c)), st_own[kind].at[s], st_sem.at[0, sem])
        return [own] if early(i) else [own, pltpu.make_async_copy(xs[kind].at[k], st_other[kind].at[s], st_sem.at[1, sem])]

    def stage_start(i):
        if not early(i):
            arrive("term", x_recv, term_groups, 0, i)
        for copy in stage(i):
            copy.start()

    def slices(kind, shape, size):
        if kind:
            r = max(16, size // shape[1])
            return shape[0] // r, lambda j: (pl.ds(pl.multiple_of(j * r, r), r), slice(None))
        cols = max(128, size // shape[0])
        return shape[1] // cols, lambda j: (slice(None), pl.ds(pl.multiple_of(j * cols, cols), cols))

    def added(dst, terms, kind, total=None):
        cuts, cut = slices(kind, dst.shape, 16384)

        def one(j, acc):
            part = cut(j)
            s = terms[0][part].astype(jnp.float32)
            for r in terms[1:]:
                s = s + r[part].astype(jnp.float32)
            s = s.astype(dst.dtype)
            dst[part] = s
            if acc is None:
                return None
            s = s.astype(jnp.float32)
            s = s * s
            s = jnp.sum(s.reshape(s.shape[0] // 8, 8, s.shape[1]), axis=0)
            for k in range(s.shape[1] // 128):
                acc = acc + s[:, k * 128 : (k + 1) * 128]
            return acc

        return lax.fori_loop(0, cuts, one, total)

    def ring(s):
        way, d, q = s
        kind, k = fresh[s] if s in fresh else arrives[(way, d + 1, q)]
        to_kind, to = arrives[s]
        group = way * len(ring_groups[1]) + ring_groups[0][items.index(s) // 2]
        return remote(landed[kind].at[k], landed[to_kind].at[to], rs_send.at[kind], rs_recv.at[group], ahead[way])

    def ring_arrive(s):
        arrive("ring", rs_recv, ring_groups, s[0], items.index(s) // 2)

    def load_state(e):
        q = pieces[e]
        part = (q[1], pl.ds(q[2] * (rows[q[0]] // PARTS), rows[q[0]] // PARTS))
        return (
            pltpu.make_async_copy(m[q[0]].at[part], kept(ms, q), in_sem.at[0, kind_of(q)]),
            pltpu.make_async_copy(v[q[0]].at[part], kept(vs, q), in_sem.at[1, kind_of(q)]),
        )

    def old(q):
        kind, k = place(q, pieces)
        return st_own[kind].at[k] if k < depth[kind] else st_other[kind].at[k - depth[kind]]

    def load_weight(q):
        return pltpu.make_async_copy(block(w, q, me), old(q), in_sem.at[2, kind_of(q)])

    window, reach = 24, 3
    for i in range(LEAD):
        lead_in(i).start()
    first = [i for i in range(len(todo)) if early(i)]
    for i in first:
        stage_start(i)
    barrier = pltpu.get_barrier_semaphore()
    for to in (partner, ahead[PLUS], ahead[MINUS]):
        pl.semaphore_signal(barrier, inc=1, device_id={"dp": to}, device_id_type=MESH)
    pl.semaphore_wait(barrier, 3)
    for i in range(window):
        if i < LEAD:
            lead_in(i).wait()
        exchange(i).start()
    total = jnp.zeros((8, 128), jnp.float32)
    for i, s in enumerate(todo):
        way, d, q = s
        kind, k = x_at[i]
        if early(i):
            arrive("term", x_recv, term_groups, 0, i)
        for copy in stage(i):
            copy.wait()
        terms = [st_own[kind].at[k % depth[kind]], st_other[kind].at[k % depth[kind]]]
        if way is not None:
            if s not in fresh:
                ring_arrive((way, d + 1, q))
                kind, k = arrives[(way, d + 1, q)]
                terms.append(landed[kind].at[k])
            else:
                kind, k = fresh[s]
            added(landed[kind].at[k], terms, kind)
            ring(s).start()
        else:
            for from_ in WAYS:
                ring_arrive((from_, 1, q))
                kind, k = arrives[(from_, 1, q)]
                terms.append(landed[kind].at[k])
            total = added(kept(own_new, q), terms, kind, total)
        if i + window < len(todo):
            exchange(i + window).start()
        if i + reach < len(todo) and not early(i + reach):
            stage_start(i + reach)
        if 12 <= i < 12 + len(pieces):
            for copy in load_state(i - 12):
                copy.start()

    squares[me] = total

    def share(j):
        return remote(squares.at[me], squares.at[me], sq_send.at[0], sq_recv.at[0], lax.rem(me + j, devices))

    def several(number, ref):
        return ref.at[pl.ds(0, number)]

    for j in sorted(range(1, devices), key=lambda j: -min(j, devices - j)):
        share(j).start()
    for q in pieces:
        load_weight(q).start()
    for kind in (0, 1):
        waited(xs[kind], x_send.at[kind])
        waited(several(sum(kind_of(s[2]) == kind for s in items), landed[kind]), rs_send.at[kind])
        for which, pair in enumerate((ms, vs, own_new)):
            waited(pair[kind], in_sem.at[which, kind])
    waited(several(devices - 1, squares), sq_recv.at[0])
    everyone = jnp.sum(jnp.sum(squares[...], axis=0), axis=(0, 1), keepdims=True)
    factor = jnp.minimum(1.0, 0.5 * lax.rsqrt(jnp.broadcast_to(everyone, (8, 128)) / count_all + 1e-30))[0:1, 0:1]

    def stepped(q, share_of=(0, 1)):
        wn, mr, vr, wr = kept(own_new, q), kept(ms, q), kept(vs, q), old(q)
        cuts, cut = slices(kind_of(q), wn.shape, 8192)

        def one(j, _):
            part = cut(j)
            grad = wn[part].astype(jnp.float32) * factor
            mm = 0.9 * mr[part] + 0.1 * grad
            vv = 0.95 * vr[part] + 0.05 * grad * grad
            mr[part] = mm
            vr[part] = vv
            before = wr[part].astype(jnp.float32)
            wn[part] = (before - 0.02 * (mm * lax.rsqrt(vv + 1e-8) + 0.1 * before)).astype(wn.dtype)
            return None

        lax.fori_loop(cuts * share_of[0] // share_of[1], cuts * (share_of[0] + 1) // share_of[1], one, None)

    gathers = [(way, h, q) for h in range(1, half) for q in pieces for way in WAYS]

    def lies(way, h, q, owner):
        if h == half - 2 and q[0] != DOWN:
            return middle[way].at[place(q, pieces)[1]]
        if h < half - 1:
            return block(t, q, owner)
        which, among = (far, far_half(way, layers)) if q in far_half(way, layers) else (near, half_of(way, layers))
        kind, k = place(q, among)
        return which[way][kind].at[k]

    def pass_on(s, columns=None):
        way, h, q = s
        owner = at(z - step[way] * (h - 1), c)
        group = way * len(gather_groups[1]) + gather_groups[0][gathers.index(s) // 2]
        src = kept(own_new, q) if h == 1 else lies(way, h - 1, q, owner)
        dst = lies(way, h, q, owner)
        if columns is not None:
            src, dst = src.at[:, columns], dst.at[:, columns]
        return remote(src, dst, ag_send.at[kind_of(q)], ag_recv.at[group], ahead[way])

    def across(q, owner, src):
        return remote(src, block(t, q, owner), y_send.at[kind_of(q)], y_recv.at[kind_of(q)], partner)

    for q in pieces:
        quarter = t[0].shape[2] // 4
        for k in range(4 if q == pieces[0] else 0):
            stepped(q, (k, 4))
            for way in WAYS:
                pass_on((way, 1, q), pl.ds(k * quarter, quarter)).start()
        if q != pieces[0]:
            stepped(q)
            for way in WAYS:
                pass_on((way, 1, q)).start()
        across(q, me, kept(own_new, q)).start()
    for i, s in enumerate(gathers):
        way, h, q = s
        owner = at(z - step[way] * h, c)
        arrive("gather", ag_recv, gather_groups, way, i // 2)
        if h + 1 < half:
            pass_on((way, h + 1, q)).start()
        if not late(n, way, h, q):
            across(q, owner, lies(way, h, q, owner)).start()
    waited(several(devices - 1, squares), sq_send.at[0])
    for kind in (0, 1):
        number = sum(kind_of(s[2]) == kind for s in gathers)
        waited(several(number, landed[kind]), ag_send.at[kind])
        number += sum(kind_of(q) == kind for q in pieces) - sum(kind_of(s[2]) == kind and late(n, *s) for s in gathers)
        waited(several(number, landed[kind]), y_send.at[kind])
        waited(several(number, landed[kind]), y_recv.at[kind])


READS = 4


def moved(sem, through=(), buf=None, direct=()):
    reads = -(-len(through) // READS)
    for j, (a, _) in enumerate(through):
        pltpu.make_async_copy(a, buf.at[j], sem.at[j // READS]).start()
    for k, (copies, _) in enumerate(direct):
        for a, b in copies:
            pltpu.make_async_copy(a, b, sem.at[reads + 1 + k]).start()
    for i in range(reads):
        these = range(i * READS, min(len(through), (i + 1) * READS))
        waited(buf.at[pl.ds(i * READS, len(these))], sem.at[i])
        for j in these:
            pltpu.make_async_copy(buf.at[j], through[j][1], sem.at[reads]).start()
    if through:
        waited(buf, sem.at[reads])
    for k, (_, total) in enumerate(direct):
        waited(total, sem.at[reads + 1 + k])


def row_part(ref, layer, part, rows, owner):
    size = rows // PARTS
    return ref.at[layer, pl.ds(pl.multiple_of(owner * rows + part * size, size), size)]


def moment_copies(pair, results, layers):
    pieces = pieces_of(layers)
    sets = [([], pair[0]), ([], pair[1])]
    for q in pieces:
        a, layer, part = q
        kind, k = place(q, pieces)
        size = results[a].shape[1] // PARTS
        sets[kind][0].append((pair[kind].at[k], results[a].at[layer, pl.ds(part * size, size)]))
    return sets


def settle(n, layers, arrays, rows, moments, middles, *refs):
    refs = list(refs)
    take = lambda number: [refs.pop(0) for _ in range(number)]
    t, own, far, near, middle = take(len(arrays)), take(1)[0], take(2), take(2), take(middles)
    pairs = [take(2) for _ in range(moments)]
    outs, results = take(len(arrays)), [take(3) for _ in range(moments)]
    buf, sem = refs
    half = n // 2
    me = lax.axis_index("dp")
    z, c = me // CORES, me % CORES
    pieces = pieces_of(layers)
    through, held = [], []
    for off in range(n):
        if off == half:
            continue
        for core in range(CORES):
            owner = lax.rem(z + off, n) * CORES + (c if core == 0 else 1 - c)
            for q in pieces:
                a, layer, part = q
                if a not in arrays:
                    continue
                dst = row_part(outs[arrays.index(a)], layer, part, rows, owner)
                src, left = None, False
                if core == 0 and off == 0:
                    src = own.at[place(q, pieces)[1]]
                for way in WAYS:
                    hops = n - off if way == PLUS else off
                    if hops == half - 1 and core == 0:
                        which, among = (far, far_half(way, layers)) if q in far_half(way, layers) else (near, half_of(way, layers))
                        src = which[way].at[place(q, among)[1]]
                    if hops == half - 2 and core == 0 and middle:
                        src = middle[way].at[place(q, pieces)[1]]
                    left = left or (core == 1 and late(n, way, hops, q))
                if left:
                    continue
                if src is not None:
                    held.append((src, dst))
                else:
                    through.append((row_part(t[arrays.index(a)], layer, part, rows, owner), dst))
    direct = [(held, buf.at[pl.ds(0, len(held))])]
    for pair, one in zip(pairs, results, strict=True):
        direct += moment_copies(pair, one, layers)
    moved(sem, through, buf, direct)


def settle_moment(layers, *refs):
    moved(refs[5], direct=moment_copies(refs[:2], refs[2:5], layers))


def complete(n, layers, arrays, rows, lates, *refs):
    k = len(arrays)
    came, crossed = refs[k : k + 4], refs[k + 4 : k + 4 + lates]
    outs, sem = refs[k + 4 + lates : 2 * k + 4 + lates], refs[2 * k + 4 + lates]
    me = lax.axis_index("dp")
    z, c = me // CORES, me % CORES
    copies = []
    for core in range(CORES):
        owner = lax.rem(z + n // 2, n) * CORES + (c if core == 0 else 1 - c)
        for way in WAYS:
            for q in far_half(way, layers):
                if q[0] in arrays:
                    src = came[2 * core + way].at[place(q, far_half(way, layers))[1]]
                    copies.append((src, row_part(outs[arrays.index(q[0])], q[1], q[2], rows, owner)))
    hops = n // 2 - 1
    for way, ref in zip(WAYS, crossed):
        owner = lax.rem(z + (n - hops if way == PLUS else hops), n) * CORES + 1 - c
        for q in pieces_of(layers):
            if late(n, way, hops, q):
                among = far_half(way, layers) if q in far_half(way, layers) else half_of(way, layers)
                copies.append((ref.at[place(q, among)[1]], row_part(outs[arrays.index(q[0])], q[1], q[2], rows, owner)))
    moved(sem, direct=[(copies, outs[0].at[0, pl.ds(0, len(copies) * (rows // PARTS))])])


def solution(mesh):
    devices = mesh.shape["dp"]
    n = devices // CORES
    hbm, vmem = pl.BlockSpec(memory_space=pltpu.HBM), pl.BlockSpec(memory_space=pltpu.VMEM)
    bf, f32 = jnp.bfloat16, jnp.float32
    dma = pltpu.SemaphoreType.DMA
    like = lambda a: jax.ShapeDtypeStruct(a.shape, a.dtype)

    def params(mib, **more):
        return pltpu.CompilerParams(vmem_limit_bytes=mib * 2**20, **more)

    def summed(terms, weights, m, v):
        layers = m[0].shape[0]
        items, finals, _, _, count = plan(n, layers)
        pieces = pieces_of(layers)
        todo = items + finals
        shapes = [(m[a].shape[1] // PARTS, m[a].shape[2]) for a in (0, DOWN)]
        pair = lambda make, number, dtype: [make((number[kind], *shapes[kind]), dtype) for kind in (0, 1)]
        whole, part = counts(pieces), counts(half_of(PLUS, layers))
        ring_groups, term_groups, gather_groups = groups_of(n, layers)
        outs = [like(w) for w in weights] + pair(jax.ShapeDtypeStruct, counts([s[2] for s in todo]), bf)
        held = 2 * pair(pltpu.VMEM, whole, f32) + pair(pltpu.VMEM, whole, bf) + 4 * pair(pltpu.VMEM, part, bf) + [pltpu.VMEM((whole[0], *shapes[0]), bf)] * 2
        return pl.pallas_call(
            functools.partial(kernel, n, devices * sum(one.size for one in m)),
            out_shape=outs + held,
            in_specs=[hbm] * 12,
            out_specs=[hbm] * len(outs) + [vmem] * len(held),
            scratch_shapes=pair(pltpu.VMEM, count, bf)
            + 2 * pair(pltpu.VMEM, [-(-number // 2) for number in whole], bf)
            + [pltpu.VMEM((devices, 8, 128), f32), pltpu.VMEM((LEAD, *shapes[0]), bf)]
            + [dma((2,)), dma((2 * len(ring_groups[1]),))]
            + [dma((2,)), dma((len(term_groups[1]),))]
            + [dma((2, sum(-(-number // 2) for number in whole)))]
            + [dma((2,)), dma((2 * len(gather_groups[1]),))]
            + [dma((2,)), dma((2,))]
            + [dma((1,)), dma((1,))]
            + [dma((3, 2)), dma((LEAD,))],
            compiler_params=params(31, collective_id=0, has_side_effects=True),
            name="summed",
        )(*terms, *weights, *m, *v)

    def settled(arrays, t, own, far, near, middle, m, moments=()):
        layers, rows = m[0].shape[0], m[arrays[0]].shape[1]
        jobs = (n - 1) * CORES * len(arrays) * layers * PARTS
        jobs -= sum(late(n, way, n // 2 - 1, q) and q[0] in arrays for way in WAYS for q in pieces_of(layers))
        held = (3 + len(middle)) * len(arrays) * layers * PARTS
        through = jobs - held
        size = rows // PARTS * t[0].shape[2]
        moved_bytes = 2 * size * (jobs + through) + sum(4 * one.size for pair in moments for one in pair)
        results = [like(one) for _ in moments for one in m]
        return pl.pallas_call(
            functools.partial(settle, n, layers, arrays, rows, len(moments), len(middle)),
            out_shape=[like(one) for one in t] + results,
            in_specs=[hbm] * len(t) + [vmem] * (5 + len(middle) + 2 * len(moments)),
            out_specs=[hbm] * (len(t) + len(results)),
            scratch_shapes=[pltpu.VMEM((through, rows // PARTS, t[0].shape[2]), bf), dma((-(-through // READS) + 2 + 2 * len(moments),))],
            compiler_params=params(-(-2 * size * through // 2**20) + 1),
            cost_estimate=pl.CostEstimate(flops=60 * moved_bytes, bytes_accessed=moved_bytes, transcendentals=0),
            name="settle",
        )(*(pltpu.with_memory_space_constraint(one, pltpu.HBM) for one in t), own, *far, *near, *middle, *(one for pair in moments for one in pair))

    def settled_moment(m, moment):
        size = 4 * sum(one.size for one in m)
        return pl.pallas_call(
            functools.partial(settle_moment, m[0].shape[0]),
            out_shape=[like(one) for one in m],
            in_specs=[vmem] * 2,
            out_specs=[hbm] * 3,
            scratch_shapes=[dma((3,))],
            compiler_params=params(8),
            cost_estimate=pl.CostEstimate(flops=60 * size, bytes_accessed=size, transcendentals=0),
            name="settle_moment",
        )(*moment)

    def completed(arrays, results, came, rows, crossed=()):
        layers = results[0].shape[0]
        return pl.pallas_call(
            functools.partial(complete, n, layers, arrays, rows, len(crossed)),
            out_shape=[like(one) for one in results],
            in_specs=[hbm] * len(results) + [vmem] * (4 + len(crossed)),
            out_specs=[hbm] * len(results),
            scratch_shapes=[dma((2,))],
            input_output_aliases={i: i for i in range(len(results))},
            compiler_params=params(8),
            name="complete",
        )(*results, *came, *crossed)

    def step(*arrays):
        terms, weights, m, v = (arrays[i : i + 3] for i in (0, 3, 6, 9))
        out = summed(terms, weights, m, v)
        t = out[:3]
        new_m, new_v, own = (out[i : i + 2] for i in (5, 7, 9))
        far, near = (out[11], out[13], out[12], out[14]), (out[15], out[17], out[16], out[18])
        middle = out[19:21]
        onward = [(i, (i + CORES) % devices) for i in range(devices)]
        back = [(b, a) for a, b in onward]
        other = [(i, i + 1 - 2 * (i % CORES)) for i in range(devices)]

        def hop(k):
            return [lax.ppermute(one, "dp", way) for one, way in zip(far[k : k + 2], (onward, back), strict=True)]

        def cross(came):
            return came + [lax.ppermute(one, "dp", other) for one in came]

        rows = [one.shape[1] for one in m]
        wide = hop(0)
        down = hop(2)
        crossed = [lax.ppermute(one, "dp", other) for one in (far[2 + PLUS], near[2 + MINUS])]
        new_g, new_u, *moments = settled((0, 1), t[:2], own[0], far[:2], near[:2], middle, m, (new_m,))
        vs = settled_moment(v, new_v)
        (new_d,) = settled((2,), t[2:], own[1], far[2:], near[2:], (), m)
        wide = cross(wide)
        down = cross(down)
        new_g, new_u = completed((0, 1), (new_g, new_u), wide, rows[0])
        (new_d,) = completed((2,), (new_d,), down, rows[2], crossed)
        return (new_g, new_u, new_d, *moments, *vs)

    all_of, cut = P(None, None, None), P(None, "dp", None)
    return jax.shard_map(
        step,
        mesh=mesh,
        in_specs=(P(("rep", "dp"), None, None, None),) * 3 + (all_of,) * 3 + (cut,) * 6,
        out_specs=(P("rep", None, None),) * 3 + (P("rep", "dp", None),) * 6,
        check_vma=False,
    )
```
